512 devices in a mesh: gy: 8 (over x, core), gx: 64 (over z, y).
Axes of the slice: x: 4, y: 8, z: 8, core: 2. Of those that a mesh axis runs over, the one named last changes fastest.
Arguments:
- position: float32 [16, 512, 128, 3], P('gy', 'gx'), may hold values from 0 to 1
- velocity: float32 [16, 512, 128, 3], P('gy', 'gx'), may hold values from -6 to 6
- particle_mass: float32 [16, 512, 128], P('gy', 'gx'), may hold values from 0.006 to 0.025
- cell_counts: int32 [16, 512], P('gy', 'gx'), may hold values from 64 to 128
- shear_shift: int32 [1], replicated, may hold values from 252 to 260
Outputs:
- density: float32 [16, 512, 128], P('gy', 'gx')
- acceleration: float32 [16, 512, 128, 3], P('gy', 'gx')
The draws below stay inside these ranges and needn't reach their ends.
Inputs may be any that keep to these rules, and one draw needn't show every extreme that they name: `shear_shift`: the offset is a whole number of cells from 252 to 260.
All inputs are finite; a program needn't handle non-finite values.
Results may differ from the reference program's by a relative error of at most 0.0003.
Values sent between devices are 32-bit elements; how exact they have to be, the bound alone decides.
No kernel may reach another device: no remote copies, remote signals or barrier semaphores. Data moves between devices by JAX's collectives and lax.ppermute only.
A program may use at most 64 MiB of HBM per device.

```python
import math
import jax
import jax.numpy as jnp
from jax import lax

SLOTS = 128
CXD = 8
NXC = 512
NYC = 16


def set_ends(result, rng, least, top_value):
    place = [jax.random.randint(jax.random.fold_in(rng, axis), (), 0, length) for axis, length in enumerate(result.shape)]
    widest = result.shape.index(max(result.shape))
    beside = place[:widest] + [(place[widest] + 1) % result.shape[widest]] + place[widest + 1:]
    return result.at[tuple(place)].set(least).at[tuple(beside)].set(top_value)


def block_levels(rng, shape, split, low, largest):
    def one(axis_at, shards_of):
        heights = jax.random.uniform(jax.random.fold_in(jax.random.fold_in(rng, 6), axis_at), (shards_of,), jnp.float32, low / len(split), largest / len(split))
        return jnp.repeat(jnp.exp(heights), shape[axis_at] // shards_of).reshape((-1,) + (1,) * (len(shape) - axis_at - 1))

    level = one(*split[0])
    for cut in split[1:]:
        level = level * one(*cut)
    return level


def gaussian(rng, extent, width, reach, split=(), kind=jnp.bfloat16):
    entries = width * jax.random.normal(rng, extent, jnp.float32)
    if split:
        entries = entries * block_levels(rng, extent, split, -0.22, 0.18)
    return jnp.clip(entries, -reach, reach).astype(kind)


def setup_inputs(seed: int = 0) -> dict:
    streams_of = jax.random.split(jax.random.key(seed), 6)
    position = jnp.clip(1.0 * jax.random.uniform(streams_of[0], (NYC, NXC, SLOTS, 3), jnp.float32) ** block_levels(streams_of[0], (NYC, NXC, SLOTS, 3), ((0, 8), (1, 64)), -0.2, 0.2), 0.0, 1.0)
    velocity = gaussian(streams_of[1], (NYC, NXC, SLOTS, 3), 1.0, 6.0, ((0, 8), (1, 64)), jnp.float32)
    particle_mass = jnp.clip(jnp.exp(math.log(0.025) - 1.4271164 * jax.random.uniform(streams_of[2], (NYC, NXC, SLOTS), jnp.float32) ** block_levels(streams_of[2], (NYC, NXC, SLOTS), ((0, 8), (1, 64)), -0.2, 0.2)), 0.006, 0.025)
    cell_counts = set_ends(jax.random.randint(streams_of[3], (NYC, NXC), SLOTS // 2, SLOTS + 1), jax.random.fold_in(streams_of[3], 1), SLOTS // 2, SLOTS).astype(jnp.int32)
    shear_shift = jax.random.randint(streams_of[4], (1,), NXC // 2 - CXD // 2, NXC // 2 + CXD // 2 + 1).astype(jnp.int32)
    return dict(position=position, velocity=velocity, particle_mass=particle_mass, cell_counts=cell_counts, shear_shift=shear_shift)


SMOOTHING = 0.5
KERNEL_NORM = 1.0 / (math.pi * SMOOTHING ** 3)
SOUND_SQ = 0.2
VISCOSITY = 0.05
SOFTENING = 0.0025
SHEAR_JUMP = 1.0

def kernel_value(dist_sq):
    distance = jnp.sqrt(dist_sq)
    ratio = distance / SMOOTHING
    inner_part = 1.0 - 1.5 * ratio * ratio + 0.75 * ratio * ratio * ratio
    outer_part = 0.25 * jnp.maximum(2.0 - ratio, 0.0) ** 3
    return KERNEL_NORM * jnp.where(ratio < 1.0, inner_part, outer_part)

def kernel_slope(dist_sq):
    distance = jnp.sqrt(dist_sq)
    ratio = distance / SMOOTHING
    inner_part = (-3.0 + 2.25 * ratio) / (SMOOTHING * SMOOTHING)
    outer_part = -0.75 * jnp.maximum(2.0 - ratio, 0.0) ** 2 / (SMOOTHING * jnp.maximum(distance, SMOOTHING))
    return KERNEL_NORM * jnp.where(ratio < 1.0, inner_part, outer_part)

def stencil(padded, row_index):
    band = lax.dynamic_slice_in_dim(padded, row_index, 3, 0)
    columns = padded.shape[1] - 2
    cell_offsets = []
    for up_down in range(3):
        for across in range(3):
            shifted = band[up_down, across:across + columns]
            cell_offsets.append(shifted)
    return jnp.concatenate(cell_offsets, axis=1)

def stencil_offsets(slots, channels, dtype):
    parts = []
    for up_down in range(3):
        for across in range(3):
            entry = jnp.array([across - 1.0, up_down - 1.0, 0.0], dtype)
            parts.append(jnp.broadcast_to(entry, (slots, 3)))
    return jnp.concatenate(parts, axis=0)

def own_cells(padded, row_index):
    return lax.dynamic_slice_in_dim(padded, row_index + 1, 1, 0)[0, 1:-1]

def pair_offsets(own_part, near_cells):
    shift_table = stencil_offsets(own_part.shape[1], near_cells.shape[-1], near_cells.dtype)
    near_pos = near_cells[:, :, 0:3] + shift_table[None]
    return own_part[:, :, None, 0:3] - near_pos[:, None, :, :]

def densities(padded):

    def one_row(row_index):
        near_cells = stencil(padded, row_index)
        own_part = own_cells(padded, row_index)
        offsets = pair_offsets(own_part, near_cells)
        dist_sq = lax.optimization_barrier(jnp.sum(offsets * offsets, axis=-1))
        return lax.optimization_barrier(jnp.sum(near_cells[:, None, :, 6] * kernel_value(dist_sq), axis=-1))
    return lax.map(one_row, jnp.arange(padded.shape[0] - 2, dtype=jnp.int32))

def forces(padded, rho_pad):
    rho_cells = rho_pad[..., None]

    def one_row(row_index):
        near_cells = stencil(padded, row_index)
        near_rho = stencil(rho_cells, row_index)[:, None, :, 0]
        own_part = own_cells(padded, row_index)
        own_rho = own_cells(rho_cells, row_index)
        offsets = pair_offsets(own_part, near_cells)
        dist_sq = lax.optimization_barrier(jnp.sum(offsets * offsets, axis=-1))
        slope = kernel_slope(dist_sq)
        near_mass = near_cells[:, None, :, 6]
        pressure_term = -(SOUND_SQ / own_rho + SOUND_SQ / near_rho) * near_mass * slope
        viscous_term = 2.0 * VISCOSITY * near_mass * slope * dist_sq / ((dist_sq + SOFTENING) * own_rho * near_rho)
        relative = own_part[:, :, None, 3:6] - near_cells[:, None, :, 3:6]
        return lax.optimization_barrier(jnp.sum(pressure_term[..., None] * offsets + viscous_term[..., None] * relative, axis=2))
    return lax.map(one_row, jnp.arange(padded.shape[0] - 2, dtype=jnp.int32))

def pad_global(fields, shift_cells, vx_jump):
    upper_rows = jnp.roll(fields[0], shift_cells, axis=0) + vx_jump
    lower_rows = jnp.roll(fields[-1], -shift_cells, axis=0) - vx_jump
    padded_y = jnp.concatenate([lower_rows[None], fields, upper_rows[None]], axis=0)
    return jnp.concatenate([padded_y[:, -1:], padded_y, padded_y[:, :1]], axis=1)

def reference(position, velocity, particle_mass, cell_counts, shear_shift):
    shift_cells = shear_shift[0]
    slots = position.shape[2]
    is_valid = jnp.arange(slots, dtype=jnp.int32)[None, None, :] < cell_counts[:, :, None]
    weight = jnp.where(is_valid, particle_mass, 0.0)
    fields = jnp.concatenate([position, velocity, weight[..., None]], axis=-1)
    vx_jump = jnp.array([0.0, 0.0, 0.0, SHEAR_JUMP, 0.0, 0.0, 0.0], fields.dtype)
    padded = pad_global(fields, shift_cells, vx_jump)
    density_raw = densities(padded)
    safe_rho = jnp.where(is_valid, density_raw, 1.0)
    rho_pad = pad_global(safe_rho[..., None], shift_cells, jnp.zeros((1,), fields.dtype))[..., 0]
    accel = forces(padded, rho_pad)
    density = jnp.where(is_valid, density_raw, 0.0)
    acceleration = jnp.where(is_valid[..., None], accel, 0.0)
    return (density, acceleration)
```

```python
import functools
import math

import jax
import jax.numpy as jnp
from jax import lax
from jax.experimental import pallas as pl
from jax.experimental.pallas import tpu as pltpu
from jax.sharding import PartitionSpec as P

SMOOTHING = 0.5
KERNEL_NORM = 1.0 / (math.pi * SMOOTHING**3)
SOUND_SQ = 0.2
VISCOSITY = 0.05
SOFTENING = 0.0025
SHEAR_JUMP = 1.0

ROWS, COLS, PLACES = 6, 12, 16
DEPTH = 32
NEAR, FAR = 7, 4
SENT = 136
BF16, F32 = jnp.bfloat16, jnp.float32
NEIGHBOURS = [(a, b) for a in (-1, 0, 1) for b in (-1, 0, 1)]
VMEM = pl.BlockSpec(memory_space=pltpu.VMEM)
SMEM = pl.BlockSpec(memory_space=pltpu.SMEM)


def pack_kernel(counts, pos, vel, mass, out):
    slot = lax.broadcasted_iota(jnp.int32, (8, 128), 1)
    column = lax.broadcasted_iota(jnp.int32, (8, 128), 0)
    for row in range(2):
        limit = jnp.zeros((8, 128), jnp.int32)
        for c in range(8):
            limit = jnp.where(column == c, counts[row, c], limit)
        out[row, 0:3] = pos[row]
        out[row, 3:6] = vel[row]
        out[row, 6] = jnp.where(slot < limit, mass[row], 0.0)


def window_kernel(info, left, own, right, same_out, far_out):
    odd, start = info[0], info[1]
    for out, shift in ((same_out, 6), (far_out, start)):
        near_row = jnp.where(odd == 1, 1, 0)
        if out is same_out:
            near_row = 1 - near_row
        place = 0
        for row, fields in ((near_row, range(NEAR)), (1 - near_row, (0, 1, 2, 6))):
            for f in fields:
                wide = jnp.concatenate([left[row, f], own[row, f], right[row, f]], axis=0)
                if out is same_out:
                    piece = wide[6:18]
                else:
                    piece = pltpu.roll(wide, 24 - shift, 0)[0:COLS]
                out[place : place + COLS, :] = piece
                place += COLS
        out[place:SENT, :] = jnp.zeros((SENT - place, 128), F32)


def parts_of(x, count):
    parts = []
    for _ in range(count - 1):
        part = x.astype(BF16).astype(F32)
        parts.append(part)
        x = x - part
    parts.append(x.astype(BF16).astype(F32))
    return parts


def main_kernel(
    info, jump_ref, left, own, right, same, far, density, accel,
    fields, jrows, irows, crows, jcols, masses, scales, rhos, dist, sums,
):
    odd, jump = info[0], jump_ref[0]

    fields[...] = jnp.zeros_like(fields)
    for row in range(2):
        for f in range(7):
            fields[2 + row, f, 0:2, :] = left[row, f, 6:8, :]
            fields[2 + row, f, 2:10, :] = own[row, f]
            fields[2 + row, f, 10:12, :] = right[row, f, 0:2, :]
    same_near = jnp.where(odd == 1, 1, 4)
    far_near = 5 - same_near
    for piece, near in ((same, same_near), (far, far_near)):
        second = jnp.where(near == 1, 0, 5)
        for f in range(NEAR):
            value = piece[f * COLS : (f + 1) * COLS, :]
            if piece is far and f == 3:
                value = value + jump
            fields[near, f, 0:COLS, :] = value
        for n, f in enumerate((0, 1, 2, 6)):
            at = (NEAR + n) * COLS
            fields[second, f, 0:COLS, :] = piece[at : at + COLS, :]

    for n, (a, b) in enumerate(NEIGHBOURS):
        k = lax.broadcasted_iota(jnp.int32, (DEPTH, 128), 0)
        scale = jnp.where(k < 18, 1.0, 0.0)
        scale = jnp.where((k >= 18) & (k < 22), float(b), scale)
        scale = jnp.where((k >= 22) & (k < 26), float(a), scale)
        scale = jnp.where(k == 26, float(a * a + b * b), scale)
        scales[0, n] = scale
        scale = jnp.where((k == 4) | (k == 10) | (k == 20) | (k == 26), float(b), 1.0)
        scale = jnp.where((k == 5) | (k == 11) | (k == 21) | (k == 27), float(a), scale)
        scales[1, n] = scale

    def build(step, carry):
        row, half = step // 2, step % 2
        base = step * (8 * DEPTH)
        one = jnp.ones((8, 128), F32)
        zero = jnp.zeros((8, 128), F32)
        cells = pl.ds(pl.multiple_of(half * 8, 8), 8)

        def put(table, k, value):
            table[pl.ds(base + k, 8, stride=DEPTH), :] = value

        norm = zero
        for f in range(3):
            x = 2.0 * fields[row, f, cells, :] - 1.0
            high, low = parts_of(x, 2)
            both = high + low
            norm = norm + both * both
            for k, (mine, other) in enumerate(((high, high), (high, low), (low, high), (low, low))):
                put(jrows, 4 * f + k, mine)
                put(irows, 4 * f + k, -2.0 * other)
            if f < 2:
                at = 18 + 4 * f
                put(jrows, at, one)
                put(jrows, at + 1, one)
                put(jrows, at + 2, high)
                put(jrows, at + 3, low)
                put(irows, at, -4.0 * high)
                put(irows, at + 1, -4.0 * low)
                put(irows, at + 2, 4.0 * one)
                put(irows, at + 3, 4.0 * one)
        for k, part in enumerate(parts_of(norm, 3)):
            put(jrows, 12 + k, part)
            put(irows, 12 + k, one)
            put(jrows, 15 + k, one)
            put(irows, 15 + k, part)
        put(jrows, 26, one)
        put(irows, 26, 4.0 * one)
        for k, part in enumerate(parts_of(fields[row, 6, cells, :], 3)):
            put(jrows, 27 + k, part)
        for k in (30, 31):
            put(jrows, k, zero)
        for k in range(27, 32):
            put(irows, k, zero)
        return carry

    lax.fori_loop(0, ROWS * 2, build, 0)

    k = lax.broadcasted_iota(jnp.int32, (DEPTH, 128), 0)
    pick_mass = jnp.where((k >= 27) & (k < 30), 1.0, 0.0).astype(BF16)

    def turn(cell, carry):
        table = jrows[pl.ds(pl.multiple_of(cell * DEPTH, DEPTH), DEPTH), :]
        flipped = table.T.astype(BF16)
        jcols[cell] = flipped
        masses[cell] = jnp.dot(flipped, pick_mass, preferred_element_type=F32)
        return carry

    def turn_row(row, carry):
        for c in range(COLS):
            turn(row * PLACES + c, carry)
        return carry

    lax.fori_loop(0, ROWS, turn_row, 0)

    def distances(cell, slot):
        table = irows[pl.ds(pl.multiple_of(cell * DEPTH, DEPTH), DEPTH), :]
        for n, (a, b) in enumerate(NEIGHBOURS):
            right_side = (table * scales[0, n]).astype(BF16)
            dist[slot, n] = jnp.dot(
                jcols[cell + a * PLACES + b], right_side, preferred_element_type=F32
            )

    def cell_of(n, columns, row0, column0):
        return (n // columns + row0) * PLACES + n % columns + column0

    def density_of(n, carry):
        cell = cell_of(n, 10, 1, 1)
        distances(cell_of(jnp.minimum(n + 1, 39), 10, 1, 1), (n + 1) % 2)
        slot = n % 2
        total = jnp.zeros((8, 128), F32)
        for m, (a, b) in enumerate(NEIGHBOURS):
            near = cell + a * PLACES + b
            for at in range(0, 128, 32):
                y = jnp.maximum(dist[slot, m, at : at + 32, :], 1e-12)
                q = y * lax.rsqrt(y)
                reach = jnp.maximum(2.0 - q, 0.0)
                inner = 4.0 - 3.0 * y * reach
                outer = reach * reach * reach
                w = jnp.where(y < 1.0, inner, outer) * masses[near, at : at + 32, :]
                total = total + ((w[0:8] + w[8:16]) + (w[16:24] + w[24:32]))
        rho = jnp.sum(total, axis=0, keepdims=True) * (0.25 * KERNEL_NORM)
        rhos[pl.ds(cell, 1), :] = rho
        return carry

    distances(cell_of(0, 10, 1, 1), 0)
    lax.fori_loop(0, 40, density_of, 0)

    def coefficients(step, carry):
        row, half = step // 2 + 1, step % 2
        base = (row * 2 + half) * (8 * DEPTH)
        cells = pl.ds(pl.multiple_of(half * 8, 8), 8)
        mass = fields[row, 6, cells, :]
        rho = rhos[pl.ds(pl.multiple_of(row * PLACES + half * 8, 8), 8), :]
        share = mass / jnp.where(mass > 0.0, rho, 1.0)
        terms = []
        for weight in (mass, share):
            terms.append(weight)
            for f in range(3):
                high, low = parts_of(2.0 * fields[row, f, cells, :] - 1.0, 2)
                terms.append(weight * (high + low))
            terms.append(weight)
            terms.append(weight)
        for f in range(3, 6):
            terms.append(share * fields[row, f, cells, :])
        terms.append(jnp.zeros((8, 128), F32))
        for t, term in enumerate(terms):
            high, low = parts_of(term, 2)
            crows[pl.ds(base + t, 8, stride=DEPTH), :] = high
            crows[pl.ds(base + 16 + t, 8, stride=DEPTH), :] = low
        return carry

    lax.fori_loop(0, 8, coefficients, 0)

    def force_of(n, carry):
        cell = cell_of(n, 8, 2, 2)
        distances(cell_of(jnp.minimum(n + 1, 15), 8, 2, 2), (n + 1) % 2)
        slot = n % 2
        total = jnp.zeros((DEPTH, 256), F32)
        for m, (a, b) in enumerate(NEIGHBOURS):
            near = cell + a * PLACES + b
            table = crows[pl.ds(pl.multiple_of(near * DEPTH, DEPTH), DEPTH), :]
            left_side = (table * scales[1, m]).astype(BF16)
            highs, lows = [], []
            for at in range(0, 128, 32):
                y = jnp.maximum(dist[slot, m, at : at + 32, :], 1e-12)
                inverse = lax.rsqrt(y)
                q = y * inverse
                reach = jnp.maximum(2.0 - q, 0.0)
                slope = jnp.where(y < 1.0, 4.0 - 3.0 * q, reach * reach * inverse)
                soft = lax.rsqrt(y + 4.0 * SOFTENING)
                damped = slope * (y * (soft * soft))
                both = jnp.concatenate([slope, damped], axis=1)
                high = both.astype(BF16)
                highs.append(high)
                lows.append((both - high.astype(F32)).astype(BF16))
            total = total + jnp.dot(
                left_side, jnp.concatenate(highs, axis=0), preferred_element_type=F32
            )
            total = total + jnp.dot(
                left_side, jnp.concatenate(lows, axis=0), preferred_element_type=F32
            )
        total = total[0:16] + total[16:32]
        for half in range(2):
            at = pl.ds(pl.multiple_of(n * 16, 16), 16)
            sums[half, at, :] = total[:, 128 * half : 128 * (half + 1)]
        return carry

    distances(cell_of(0, 8, 2, 2), 0)
    lax.fori_loop(0, 16, force_of, 0)

    for row in range(2):
        mass = fields[2 + row, 6, 2:10, :]
        valid = mass > 0.0
        rho = rhos[(2 + row) * PLACES + 2 : (2 + row) * PLACES + 10, :]
        density[row] = jnp.where(valid, rho, 0.0)
        inverse_rho = 1.0 / jnp.where(valid, rho, 1.0)

        def term(k, half):
            return sums[half, pl.ds(row * 128 + k, 8, stride=16), :]

        mass_sum, share_sum, drag_sum = term(0, 0), term(6, 0), term(6, 1)
        pressure_scale = -3.0 * KERNEL_NORM * -SOUND_SQ * 0.5
        viscous_scale = -3.0 * KERNEL_NORM * 2.0 * VISCOSITY
        for f in range(3):
            high, low = parts_of(2.0 * fields[2 + row, f, 2:10, :] - 1.0, 2)
            x = high + low
            first = x * mass_sum - term(1 + f, 0)
            second = x * share_sum - term(7 + f, 0)
            if f < 2:
                first = first - 2.0 * term(4 + f, 0)
                second = second - 2.0 * term(10 + f, 0)
            viscous = fields[2 + row, 3 + f, 2:10, :] * drag_sum - term(12 + f, 1)
            value = pressure_scale * (first * inverse_rho + second)
            value = value + viscous_scale * viscous * inverse_rho
            accel[row, f] = jnp.where(valid, value, 0.0)


def local(rows_axis, columns_axis, position, velocity, particle_mass, cell_counts, shear_shift):
    slabs, blocks = lax.axis_size(rows_axis), lax.axis_size(columns_axis)
    axes = (rows_axis, columns_axis)
    half = blocks // 2
    slab = lax.axis_index(rows_axis)
    past = shear_shift[0] - half * particle_mass.shape[1]

    fields = pl.pallas_call(
        pack_kernel,
        out_shape=jax.ShapeDtypeStruct((2, 7, 8, 128), F32),
        in_specs=[SMEM, VMEM, VMEM, VMEM],
        out_specs=VMEM,
        name="pack",
    )(
        cell_counts,
        jnp.transpose(position, (0, 3, 1, 2)),
        jnp.transpose(velocity, (0, 3, 1, 2)),
        particle_mass,
    )
    ring = [(i, (i + 1) % blocks) for i in range(blocks)]
    left = lax.ppermute(fields, columns_axis, ring)
    right = lax.ppermute(fields, columns_axis, [(j, i) for i, j in ring])

    odd = lax.rem(slab, 2)
    start = 6 + jnp.where(slab == slabs - 1, past, jnp.where(slab == 0, -past, 0))
    info = jnp.stack([odd, start]).astype(jnp.int32)
    sent = jax.ShapeDtypeStruct((SENT, 128), F32)
    same, far = pl.pallas_call(
        window_kernel,
        out_shape=(sent, sent),
        in_specs=[SMEM, VMEM, VMEM, VMEM],
        out_specs=(VMEM, VMEM),
        name="window",
    )(info, left, fields, right)

    same_pairs, far_pairs = [], []
    for s in range(slabs):
        for b in range(blocks):
            me = s * blocks + b
            same_pairs.append((me, (s + 1 if s % 2 == 0 else s - 1) * blocks + b))
            other, to = (s - 1, b) if s % 2 == 0 else (s + 1, b)
            if other < 0 or other >= slabs:
                other, to = other % slabs, (b + half) % blocks
            far_pairs.append((me, other * blocks + to))
    far = lax.ppermute(far, axes, far_pairs)
    same = lax.ppermute(same, axes, same_pairs)

    jump = jnp.where(slab == slabs - 1, SHEAR_JUMP, jnp.where(slab == 0, -SHEAR_JUMP, 0.0))
    cells = ROWS * PLACES
    density, accel = pl.pallas_call(
        main_kernel,
        out_shape=(
            jax.ShapeDtypeStruct((2, 8, 128), F32),
            jax.ShapeDtypeStruct((2, 3, 8, 128), F32),
        ),
        in_specs=[SMEM, SMEM] + [VMEM] * 5,
        out_specs=(VMEM, VMEM),
        scratch_shapes=[
            pltpu.VMEM((ROWS, 7, PLACES, 128), F32),
            pltpu.VMEM((cells * DEPTH, 128), F32),
            pltpu.VMEM((cells * DEPTH, 128), F32),
            pltpu.VMEM((cells * DEPTH, 128), F32),
            pltpu.VMEM((cells, 128, DEPTH), BF16),
            pltpu.VMEM((cells, 128, 128), F32),
            pltpu.VMEM((2, 9, DEPTH, 128), F32),
            pltpu.VMEM((cells, 128), F32),
            pltpu.VMEM((2, 9, 128, 128), F32),
            pltpu.VMEM((2, 16 * 16, 128), F32),
        ],
        name="particles",
    )(info, jump.astype(F32)[None], left, fields, right, same, far)
    return (density, jnp.transpose(accel, (0, 2, 3, 1)))


def solution(mesh):
    placed = (
        P("gy", "gx", None, None),
        P("gy", "gx", None, None),
        P("gy", "gx", None),
        P("gy", "gx"),
        P(),
    )
    return jax.shard_map(
        functools.partial(local, "gy", "gx"),
        mesh=mesh,
        in_specs=placed,
        out_specs=(P("gy", "gx", None), P("gy", "gx", None, None)),
        check_vma=False,
    )
```

```python
import functools
import math

import jax
import jax.numpy as jnp
from jax import lax
from jax.experimental import pallas as pl
from jax.experimental.pallas import tpu as pltpu
from jax.sharding import PartitionSpec as P

SMOOTHING = 0.5
KERNEL_NORM = 1.0 / (math.pi * SMOOTHING**3)
SOUND_SQ = 0.2
VISCOSITY = 0.05
SOFTENING = 0.0025
SHEAR_JUMP = 1.0

COLS, PLACES = 12, 16
DEPTH = 32
NEAR, FAR = 7, 4
SENT = 136
BF16, F32 = jnp.bfloat16, jnp.float32
NEIGHBOURS = [(a, b) for a in (-1, 0, 1) for b in (-1, 0, 1)]
VMEM = pl.BlockSpec(memory_space=pltpu.VMEM)
SMEM = pl.BlockSpec(memory_space=pltpu.SMEM)
HBM = pl.BlockSpec(memory_space=pltpu.HBM)
TABLES = (
    jax.ShapeDtypeStruct((2, 7, PLACES, 128), F32),
    jax.ShapeDtypeStruct((2 * PLACES * DEPTH, 128), F32),
    jax.ShapeDtypeStruct((2 * PLACES, 128, DEPTH), BF16),
    jax.ShapeDtypeStruct((2 * PLACES, 128, 128), F32),
)


def pack_kernel(counts, pos_hbm, vel_hbm, mass_hbm, out, pos, vel, mass, sems):
    copies = [
        pltpu.make_async_copy(source, to, sems.at[n])
        for n, (source, to) in enumerate(((pos_hbm, pos), (vel_hbm, vel), (mass_hbm, mass)))
    ]
    for copy in copies:
        copy.start()
    slot = lax.broadcasted_iota(jnp.int32, (8, 128), 1)
    column = lax.broadcasted_iota(jnp.int32, (8, 128), 0)
    limits = []
    for row in range(2):
        limit = jnp.zeros((8, 128), jnp.int32)
        for c in range(8):
            limit = jnp.where(column == c, counts[row, c], limit)
        limits.append(limit)
    for copy in copies:
        copy.wait()
    for row in range(2):
        out[row, 0:3] = pos[row]
        out[row, 3:6] = vel[row]
        out[row, 6] = jnp.where(slot < limits[row], mass[row], 0.0)


def window_kernel(info, left, own, right, far_out, same_out):
    odd, start = info[0], info[1]
    for out in (far_out, same_out):
        near_row = jnp.where(odd == 1, 1, 0)
        if out is same_out:
            near_row = 1 - near_row
        place = 0
        for row, fields in ((near_row, range(NEAR)), (1 - near_row, (0, 1, 2, 6))):
            for f in fields:
                wide = jnp.concatenate([left[row, f], own[row, f], right[row, f]], axis=0)
                if out is same_out:
                    piece = wide[6:18]
                else:
                    piece = pltpu.roll(wide, 24 - start, 0)[0:COLS]
                out[place : place + COLS, :] = piece
                place += COLS
        out[place:SENT, :] = jnp.zeros((SENT - place, 128), F32)


def parts_of(x, count):
    parts = []
    for _ in range(count - 1):
        part = x.astype(BF16).astype(F32)
        parts.append(part)
        x = x - part
    parts.append(x.astype(BF16).astype(F32))
    return parts


def fill_scales(scales):
    k = lax.broadcasted_iota(jnp.int32, (DEPTH, 128), 0)
    for n, (a, b) in enumerate(NEIGHBOURS):
        scale = jnp.where(k < 18, 1.0, 0.0)
        scale = jnp.where((k >= 18) & (k < 22), float(b), scale)
        scale = jnp.where((k >= 22) & (k < 26), float(a), scale)
        scale = jnp.where(k == 26, float(a * a + b * b), scale)
        scales[0, n] = scale
        if scales.shape[0] > 1:
            scale = jnp.where((k == 4) | (k == 10) | (k == 20) | (k == 26), float(b), 1.0)
            scale = jnp.where((k == 5) | (k == 11) | (k == 21) | (k == 27), float(a), scale)
            scales[1, n] = scale


def build_tables(rows, fields, irows, jcols, masses, jrows):
    k = lax.broadcasted_iota(jnp.int32, (DEPTH, 128), 0)
    ones_j = jnp.where(((k >= 15) & (k < 20)) | (k == 22) | (k == 23) | (k == 26), 1.0, 0.0)
    ones_i = jnp.where((k >= 12) & (k < 15), 1.0, 0.0)
    ones_i = jnp.where((k == 20) | (k == 21) | (k >= 24) & (k < 27), 4.0, ones_i)
    pick_mass = jnp.where((k >= 27) & (k < 30), 1.0, 0.0).astype(BF16)

    def build(step, carry):
        row, half = step // 2, step % 2
        base = pl.multiple_of(step * (8 * DEPTH), 8 * DEPTH)
        cells = pl.ds(pl.multiple_of(half * 8, 8), 8)
        for c in range(8):
            jrows[pl.ds(base + c * DEPTH, DEPTH), :] = ones_j
            irows[pl.ds(base + c * DEPTH, DEPTH), :] = ones_i

        def put(table, k, value):
            table[pl.ds(base + k, 8, stride=DEPTH), :] = value

        norm = jnp.zeros((8, 128), F32)
        for f in range(3):
            x = 2.0 * fields[row, f, cells, :] - 1.0
            high, low = parts_of(x, 2)
            both = high + low
            norm = norm + both * both
            for k, (mine, other) in enumerate(((high, high), (high, low), (low, high), (low, low))):
                put(jrows, 4 * f + k, mine)
                put(irows, 4 * f + k, -2.0 * other)
            if f < 2:
                at = 18 + 4 * f
                put(jrows, at + 2, high)
                put(jrows, at + 3, low)
                put(irows, at, -4.0 * high)
                put(irows, at + 1, -4.0 * low)
        for k, part in enumerate(parts_of(norm, 3)):
            put(jrows, 12 + k, part)
            put(irows, 15 + k, part)
        for k, part in enumerate(parts_of(fields[row, 6, cells, :], 3)):
            put(jrows, 27 + k, part)
        return carry

    lax.fori_loop(0, rows * 2, build, 0)

    def turn_row(row, carry):
        for c in range(COLS):
            cell = row * PLACES + c
            table = jrows[pl.ds(pl.multiple_of(cell * DEPTH, DEPTH), DEPTH), :]
            flipped = table.T.astype(BF16)
            jcols[cell] = flipped
            masses[cell] = jnp.dot(flipped, pick_mass, preferred_element_type=F32)
        return carry

    lax.fori_loop(0, rows, turn_row, 0)


def rows_of(table, cell):
    return table[pl.ds(pl.multiple_of(cell * DEPTH, DEPTH), DEPTH), :]


def put_distances(dist, m, table, scale, columns):
    right_side = (table * scale).astype(BF16)
    dist[m] = jnp.dot(columns, right_side, preferred_element_type=F32)


def add_density(total, dist, m, masses, cell):
    for at in range(0, 128, 32):
        y = jnp.maximum(dist[m, at : at + 32, :], 1e-12)
        q = y * lax.rsqrt(y)
        reach = jnp.maximum(2.0 - q, 0.0)
        inner = 4.0 - 3.0 * y * reach
        outer = reach * reach * reach
        w = jnp.where(y < 1.0, inner, outer) * masses[cell, at : at + 32, :]
        total = total + ((w[0:8] + w[8:16]) + (w[16:24] + w[24:32]))
    return total


def density_of(total):
    return jnp.sum(total, axis=0, keepdims=True) * (0.25 * KERNEL_NORM)


def row_index(direction, b):
    return direction * 3 + b + 1


def early_kernel(left, own, right, fields, irows, jcols, masses, rhos, jrows, scales, dist):
    fields[...] = jnp.zeros_like(fields)
    for row in range(2):
        for f in range(7):
            fields[row, f, 0:2, :] = left[row, f, 6:8, :]
            fields[row, f, 2:10, :] = own[row, f]
            fields[row, f, 10:12, :] = right[row, f, 0:2, :]
    fill_scales(scales)
    build_tables(2, fields, irows, jcols, masses, jrows)

    def blocks(n):
        side, column = n // 10, n % 10 + 1
        cell = side * PLACES + column
        other = (1 - side) * PLACES + column
        return cell, [
            (row_index(direction, b), at + b)
            for direction, at in ((1, cell), (2 - 2 * side, other))
            for b in (-1, 0, 1)
        ]

    def measure(n, m):
        cell, near = blocks(n)
        put_distances(dist, m, rows_of(irows, cell), scales[0, near[m][0]], jcols[near[m][1]])

    def step(n, carry):
        cell, near = blocks(n)
        following = jnp.minimum(n + 1, 19)
        total = jnp.zeros((8, 128), F32)
        for m in range(6):
            total = add_density(total, dist, m, masses, near[m][1])
            measure(following, m)
        rhos[pl.ds(cell, 1), :] = density_of(total)
        return carry

    rhos[...] = jnp.zeros_like(rhos)
    for m in range(6):
        measure(0, m)
    lax.fori_loop(0, 20, step, 0)


def late_kernel(
    info, jump_ref, far, same, fields, irows, jcols, masses, partial, density, accel,
    ghosts, ghost_irows, ghost_jcols, ghost_masses, jrows,
    scales, rhos, ghost_rhos, crows, ghost_crows, dist, sums,
):
    odd, jump = info[0], jump_ref[0]

    ghosts[...] = jnp.zeros_like(ghosts)
    for piece, side in ((same, 1 - odd), (far, odd)):
        for f in range(NEAR):
            value = piece[f * COLS : (f + 1) * COLS, :]
            if piece is far and f == 3:
                value = value + jump
            ghosts[side, f, 0:COLS, :] = value
        for n, f in enumerate((0, 1, 2, 6)):
            at = (NEAR + n) * COLS
            ghosts[2 + side, f, 0:COLS, :] = piece[at : at + COLS, :]
    fill_scales(scales)
    build_tables(4, ghosts, ghost_irows, ghost_jcols, ghost_masses, jrows)

    def blocks(n):
        side, column = n // 10, n % 10 + 1
        cell = side * PLACES + column
        return cell, side, [
            (who, row_index(direction, b), at + b)
            for who, direction, at in (
                ("far", 2 * side, cell + 2 * PLACES),
                ("near", 1, cell),
                ("own", 2 - 2 * side, cell),
                ("mine", 2 * side, cell),
            )
            for b in (-1, 0, 1)
        ]

    def measure(n, m):
        cell, side, near = blocks(n)
        who, index, at = near[m]
        table = rows_of(irows if who == "mine" else ghost_irows, cell)
        columns = (jcols if who == "own" else ghost_jcols)[at]
        put_distances(dist, m, table, scales[0, index], columns)

    def density_step(n, carry):
        cell, side, near = blocks(n)
        following = jnp.minimum(n + 1, 19)
        ghost_total = jnp.zeros((8, 128), F32)
        own_total = jnp.zeros((8, 128), F32)
        for m in range(12):
            who, index, at = near[m]
            which = masses if who == "own" else ghost_masses
            if who == "mine":
                own_total = add_density(own_total, dist, m, which, at)
            else:
                ghost_total = add_density(ghost_total, dist, m, which, at)
            measure(following, m)
        ghost_rhos[pl.ds(cell, 1), :] = density_of(ghost_total)
        rhos[pl.ds(cell, 1), :] = density_of(own_total) + partial[pl.ds(cell, 1), :]
        return carry

    rhos[...] = jnp.zeros_like(rhos)
    ghost_rhos[...] = jnp.zeros_like(ghost_rhos)
    for m in range(12):
        measure(0, m)
    lax.fori_loop(0, 20, density_step, 0)

    def coefficients(source, densities, target):
        def step(n, carry):
            row, half = n // 2, n % 2
            base = n * (8 * DEPTH)
            cells = pl.ds(pl.multiple_of(half * 8, 8), 8)
            mass = source[row, 6, cells, :]
            rho = densities[pl.ds(pl.multiple_of(n * 8, 8), 8), :]
            share = mass / jnp.where(mass > 0.0, rho, 1.0)
            terms = []
            for weight in (mass, share):
                terms.append(weight)
                for f in range(3):
                    high, low = parts_of(2.0 * source[row, f, cells, :] - 1.0, 2)
                    terms.append(weight * (high + low))
                terms.append(weight)
                terms.append(weight)
            for f in range(3, 6):
                terms.append(share * source[row, f, cells, :])
            terms.append(jnp.zeros((8, 128), F32))
            for t, term in enumerate(terms):
                high, low = parts_of(term, 2)
                target[pl.ds(base + t, 8, stride=DEPTH), :] = high
                target[pl.ds(base + 16 + t, 8, stride=DEPTH), :] = low
            return carry

        lax.fori_loop(0, 4, step, 0)

    coefficients(fields, rhos, crows)
    coefficients(ghosts, ghost_rhos, ghost_crows)

    def force_blocks(n):
        side, column = n // 8, n % 8 + 2
        cell = side * PLACES + column
        other = (1 - side) * PLACES + column
        return cell, [
            (ghost, row_index(direction, b), at + b)
            for ghost, direction, at in (
                (True, 2 * side, cell),
                (False, 1, cell),
                (False, 2 - 2 * side, other),
            )
            for b in (-1, 0, 1)
        ]

    def force_measure(n, m):
        cell, near = force_blocks(n)
        ghost, index, at = near[m]
        columns = (ghost_jcols if ghost else jcols)[at]
        put_distances(dist, m, rows_of(irows, cell), scales[0, index], columns)

    def force_step(n, carry):
        cell, near = force_blocks(n)
        following = jnp.minimum(n + 1, 15)
        total = jnp.zeros((DEPTH, 256), F32)
        for m in range(9):
            ghost, index, at = near[m]
            table = rows_of(ghost_crows if ghost else crows, at)
            left_side = (table * scales[1, index]).astype(BF16)
            highs, lows = [], []
            for at in range(0, 128, 32):
                y = jnp.maximum(dist[m, at : at + 32, :], 1e-12)
                inverse = lax.rsqrt(y)
                q = y * inverse
                reach = jnp.maximum(2.0 - q, 0.0)
                slope = jnp.where(y < 1.0, 4.0 - 3.0 * q, reach * reach * inverse)
                soft = lax.rsqrt(y + 4.0 * SOFTENING)
                damped = slope * (y * (soft * soft))
                both = jnp.concatenate([slope, damped], axis=1)
                high = both.astype(BF16)
                highs.append(high)
                lows.append((both - high.astype(F32)).astype(BF16))
            force_measure(following, m)
            total = total + jnp.dot(
                left_side, jnp.concatenate(highs, axis=0), preferred_element_type=F32
            )
            total = total + jnp.dot(
                left_side, jnp.concatenate(lows, axis=0), preferred_element_type=F32
            )
        total = total[0:16] + total[16:32]
        for half in range(2):
            at = pl.ds(pl.multiple_of(n * 16, 16), 16)
            sums[half, at, :] = total[:, 128 * half : 128 * (half + 1)]
        return carry

    for m in range(9):
        force_measure(0, m)
    lax.fori_loop(0, 16, force_step, 0)

    for row in range(2):
        mass = fields[row, 6, 2:10, :]
        valid = mass > 0.0
        rho = rhos[row * PLACES + 2 : row * PLACES + 10, :]
        density[row] = jnp.where(valid, rho, 0.0)
        inverse_rho = 1.0 / jnp.where(valid, rho, 1.0)

        def term(k, half):
            return sums[half, pl.ds(row * 128 + k, 8, stride=16), :]

        mass_sum, share_sum, drag_sum = term(0, 0), term(6, 0), term(6, 1)
        pressure_scale = -3.0 * KERNEL_NORM * -SOUND_SQ * 0.5
        viscous_scale = -3.0 * KERNEL_NORM * 2.0 * VISCOSITY
        for f in range(3):
            high, low = parts_of(2.0 * fields[row, f, 2:10, :] - 1.0, 2)
            x = high + low
            first = x * mass_sum - term(1 + f, 0)
            second = x * share_sum - term(7 + f, 0)
            if f < 2:
                first = first - 2.0 * term(4 + f, 0)
                second = second - 2.0 * term(10 + f, 0)
            viscous = fields[row, 3 + f, 2:10, :] * drag_sum - term(12 + f, 1)
            value = pressure_scale * (first * inverse_rho + second)
            value = value + viscous_scale * viscous * inverse_rho
            accel[row, f] = jnp.where(valid, value, 0.0)


def scratch_of(tables, rows):
    return [
        pltpu.VMEM((t.shape[0] // 2 * rows, *t.shape[1:]), t.dtype) for t in tables
    ]


def params(mib):
    return pltpu.CompilerParams(vmem_limit_bytes=mib * 2**20)


def local(rows_axis, columns_axis, position, velocity, particle_mass, cell_counts, shear_shift):
    slabs, blocks = lax.axis_size(rows_axis), lax.axis_size(columns_axis)
    axes = (rows_axis, columns_axis)
    half = blocks // 2
    slab = lax.axis_index(rows_axis)
    past = shear_shift[0] - half * particle_mass.shape[1]

    fields = pl.pallas_call(
        pack_kernel,
        out_shape=jax.ShapeDtypeStruct((2, 7, 8, 128), F32),
        in_specs=[SMEM, HBM, HBM, HBM],
        out_specs=VMEM,
        scratch_shapes=[
            pltpu.VMEM((2, 3, 8, 128), F32),
            pltpu.VMEM((2, 3, 8, 128), F32),
            pltpu.VMEM((2, 8, 128), F32),
            pltpu.SemaphoreType.DMA((3,)),
        ],
        name="pack",
    )(
        cell_counts,
        jnp.transpose(position, (0, 3, 1, 2)),
        jnp.transpose(velocity, (0, 3, 1, 2)),
        particle_mass,
    )
    ring = [(i, (i + 1) % blocks) for i in range(blocks)]
    left = lax.ppermute(fields, columns_axis, ring)
    right = lax.ppermute(fields, columns_axis, [(j, i) for i, j in ring])

    odd = lax.rem(slab, 2)
    start = 6 + jnp.where(slab == slabs - 1, past, jnp.where(slab == 0, -past, 0))
    info = jnp.stack([odd, start]).astype(jnp.int32)
    sent = jax.ShapeDtypeStruct((SENT, 128), F32)
    far, same = pl.pallas_call(
        window_kernel,
        out_shape=(sent, sent),
        in_specs=[SMEM, VMEM, VMEM, VMEM],
        out_specs=(VMEM, VMEM),
        compiler_params=params(4),
        name="window",
    )(info, left, fields, right)

    same_pairs, far_pairs = [], []
    for s in range(slabs):
        for b in range(blocks):
            me = s * blocks + b
            same_pairs.append((me, (s + 1 if s % 2 == 0 else s - 1) * blocks + b))
            other, to = (s - 1, b) if s % 2 == 0 else (s + 1, b)
            if other < 0 or other >= slabs:
                other, to = other % slabs, (b + half) % blocks
            far_pairs.append((me, other * blocks + to))
    far = lax.ppermute(far, axes, far_pairs)
    same = lax.ppermute(same, axes, same_pairs)

    tables = pl.pallas_call(
        early_kernel,
        out_shape=(*TABLES, jax.ShapeDtypeStruct((2 * PLACES, 128), F32)),
        in_specs=[VMEM] * 3,
        out_specs=[VMEM] * 5,
        scratch_shapes=[
            pltpu.VMEM((2 * PLACES * DEPTH, 128), F32),
            pltpu.VMEM((1, 9, DEPTH, 128), F32),
            pltpu.VMEM((6, 128, 128), F32),
        ],
        compiler_params=params(8),
        cost_estimate=pl.CostEstimate(
            flops=400_000_000, bytes_accessed=4_000_000, transcendentals=2_000_000
        ),
        name="early",
    )(left, fields, right)

    jump = jnp.where(slab == slabs - 1, SHEAR_JUMP, jnp.where(slab == 0, -SHEAR_JUMP, 0.0))
    density, accel = pl.pallas_call(
        late_kernel,
        out_shape=(
            jax.ShapeDtypeStruct((2, 8, 128), F32),
            jax.ShapeDtypeStruct((2, 3, 8, 128), F32),
        ),
        in_specs=[SMEM, SMEM] + [VMEM] * 7,
        out_specs=(VMEM, VMEM),
        scratch_shapes=[
            *scratch_of(TABLES, 4),
            pltpu.VMEM((4 * PLACES * DEPTH, 128), F32),
            pltpu.VMEM((2, 9, DEPTH, 128), F32),
            pltpu.VMEM((2 * PLACES, 128), F32),
            pltpu.VMEM((2 * PLACES, 128), F32),
            pltpu.VMEM((2 * PLACES * DEPTH, 128), F32),
            pltpu.VMEM((2 * PLACES * DEPTH, 128), F32),
            pltpu.VMEM((12, 128, 128), F32),
            pltpu.VMEM((2, 16 * 16, 128), F32),
        ],
        compiler_params=params(24),
        name="late",
    )(info, jump.astype(F32)[None], far, same, *tables)
    return (density, jnp.transpose(accel, (0, 2, 3, 1)))


def solution(mesh):
    placed = (
        P("gy", "gx", None, None),
        P("gy", "gx", None, None),
        P("gy", "gx", None),
        P("gy", "gx"),
        P(),
    )
    return jax.shard_map(
        functools.partial(local, "gy", "gx"),
        mesh=mesh,
        in_specs=placed,
        out_specs=(P("gy", "gx", None), P("gy", "gx", None, None)),
        check_vma=False,
    )
```

```python
import math

import jax
import jax.numpy as jnp
from jax import lax
from jax.experimental import pallas as pl
from jax.experimental.pallas import tpu as pltpu
from jax.sharding import PartitionSpec as P


SMOOTHING = 0.5
KERNEL_NORM = 1.0 / (math.pi * SMOOTHING**3)
SOUND_SQ = 0.2
VISCOSITY = 0.05
SOFTENING = 0.0025
SHEAR_JUMP = 1.0

COLS, PLACES = 12, 16
DEPTH = 32
NEAR = 7
SENT = 136
BF16, F32 = jnp.bfloat16, jnp.float32
NEIGHBOURS = [(a, b) for a in (-1, 0, 1) for b in (-1, 0, 1)]
VMEM = pl.BlockSpec(memory_space=pltpu.VMEM)
SMEM = pl.BlockSpec(memory_space=pltpu.SMEM)
TABLES = (
    jax.ShapeDtypeStruct((2, 7, PLACES, 128), F32),
    jax.ShapeDtypeStruct((2 * PLACES * DEPTH, 128), F32),
    jax.ShapeDtypeStruct((2 * COLS, 128, DEPTH), BF16),
    jax.ShapeDtypeStruct((2 * COLS, 128, 128), F32),
)


def place_of(column):
    return jnp.where(column < 0, column + 10, jnp.where(column > 7, column + 2, column))


def window_kernel(info, left, own, right, far_out, same_out):
    odd, start = info[0], info[1]
    for out in (far_out, same_out):
        near_row = jnp.where(odd == 1, 1, 0)
        if out is same_out:
            near_row = 1 - near_row
        place = 0
        for row, fields in ((near_row, range(NEAR)), (1 - near_row, (0, 1, 2, 6))):
            for f in fields:
                wide = jnp.concatenate([left[row, f], own[row, f], right[row, f]], axis=0)
                if out is same_out:
                    piece = wide[6:18]
                else:
                    piece = pltpu.roll(wide, 24 - start, 0)[0:COLS]
                out[place : place + COLS, :] = piece
                place += COLS
        out[place:SENT, :] = jnp.zeros((SENT - place, 128), F32)


def parts_of(x, count):
    parts = []
    for _ in range(count - 1):
        part = x.astype(BF16).astype(F32)
        parts.append(part)
        x = x - part
    parts.append(x.astype(BF16).astype(F32))
    return parts


def fill_scales(scales):
    k = lax.broadcasted_iota(jnp.int32, (DEPTH, 128), 0)
    for n, (a, b) in enumerate(NEIGHBOURS):
        scale = jnp.where(k < 18, 1.0, 0.0)
        scale = jnp.where((k >= 18) & (k < 22), float(b), scale)
        scale = jnp.where((k >= 22) & (k < 26), float(a), scale)
        scale = jnp.where(k == 26, float(a * a + b * b), scale)
        scales[0, n] = scale
        if scales.shape[0] > 1:
            scale = jnp.where((k == 4) | (k == 10) | (k == 20) | (k == 26), float(b), 1.0)
            scale = jnp.where((k == 5) | (k == 11) | (k == 21) | (k == 27), float(a), scale)
            scales[1, n] = scale


def build_tables(rows, halves, fields, irows, jcols, masses, jrows):
    k = lax.broadcasted_iota(jnp.int32, (DEPTH, 128), 0)
    ones_j = jnp.where(((k >= 15) & (k < 20)) | (k == 22) | (k == 23) | (k == 26), 1.0, 0.0)
    ones_i = jnp.where((k >= 12) & (k < 15), 1.0, 0.0)
    ones_i = jnp.where((k == 20) | (k == 21) | (k >= 24) & (k < 27), 4.0, ones_i)
    pick_mass = jnp.where((k >= 27) & (k < 30), 1.0, 0.0).astype(BF16)

    count = len(halves)

    def build(n, carry):
        row, half = n // count, n % count + halves[0]
        step = row * 2 + half
        base = pl.multiple_of(step * (8 * DEPTH), 8 * DEPTH)
        cells = pl.ds(pl.multiple_of(half * 8, 8), 8)
        for c in range(8):
            jrows[pl.ds(base + c * DEPTH, DEPTH), :] = ones_j
            irows[pl.ds(base + c * DEPTH, DEPTH), :] = ones_i

        def put(table, k, value):
            table[pl.ds(base + k, 8, stride=DEPTH), :] = value

        norm = jnp.zeros((8, 128), F32)
        for f in range(3):
            x = 2.0 * fields[row, f, cells, :] - 1.0
            high, low = parts_of(x, 2)
            both = high + low
            norm = norm + both * both
            for k, (mine, other) in enumerate(((high, high), (high, low), (low, high), (low, low))):
                put(jrows, 4 * f + k, mine)
                put(irows, 4 * f + k, -2.0 * other)
            if f < 2:
                at = 18 + 4 * f
                put(jrows, at + 2, high)
                put(jrows, at + 3, low)
                put(irows, at, -4.0 * high)
                put(irows, at + 1, -4.0 * low)
        for k, part in enumerate(parts_of(norm, 3)):
            put(jrows, 12 + k, part)
            put(irows, 15 + k, part)
        for k, part in enumerate(parts_of(fields[row, 6, cells, :], 3)):
            put(jrows, 27 + k, part)
        return carry

    lax.fori_loop(0, rows * count, build, 0)

    def turn_row(row, carry):
        for c in range(8 * halves[0], 8 if halves[-1] == 0 else COLS):
            cell = row * PLACES + c
            table = jrows[pl.ds(pl.multiple_of(cell * DEPTH, DEPTH), DEPTH), :]
            flipped = table.T.astype(BF16)
            jcols[row * COLS + c] = flipped
            masses[row * COLS + c] = jnp.dot(flipped, pick_mass, preferred_element_type=F32)
        return carry

    lax.fori_loop(0, rows, turn_row, 0)


def packed(cell):
    return cell - (PLACES - COLS) * (cell // PLACES)


def rows_of(table, cell):
    return table[pl.ds(pl.multiple_of(cell * DEPTH, DEPTH), DEPTH), :]


def put_distances(dist, m, table, scale, columns):
    right_side = (table * scale).astype(BF16)
    dist[m] = jnp.dot(columns, right_side, preferred_element_type=F32)


def add_density(total, dist, m, masses, cell):
    cell = packed(cell)
    for at in range(0, 128, 32):
        y = jnp.maximum(dist[m, at : at + 32, :], 1e-12)
        q = y * lax.rsqrt(y)
        reach = jnp.maximum(2.0 - q, 0.0)
        inner = 4.0 - 3.0 * y * reach
        outer = reach * reach * reach
        w = jnp.where(y < 1.0, inner, outer) * masses[cell, at : at + 32, :]
        total = total + ((w[0:8] + w[8:16]) + (w[16:24] + w[24:32]))
    return total


def density_of(total):
    return jnp.sum(total, axis=0, keepdims=True) * (0.25 * KERNEL_NORM)


def row_index(direction, b):
    return direction * 3 + b + 1


def own_kernel(run, own, *refs):
    fields, irows, jcols, masses, rhos, jrows, scales, dist = refs[-8:]

    @pl.when(run[0] == 1)
    def _():
        fields[...] = jnp.zeros_like(fields)
        for row in range(2):
            for f in range(7):
                fields[row, f, 0:8, :] = own[row, f]
        fill_scales(scales)
        build_tables(2, (0,), fields, irows, jcols, masses, jrows)
        jcols[8] = jnp.zeros((128, DEPTH), BF16)
        masses[8] = jnp.zeros((128, 128), F32)

        def blocks(n):
            side, column = n // 8, n % 8
            found = []
            for direction, row in ((1, side), (2 - 2 * side, 1 - side)):
                for b in (-1, 0, 1):
                    at = column + b
                    inside = (at >= 0) & (at < 8)
                    found.append(
                        (row_index(direction, b), jnp.where(inside, row * PLACES + at, 8))
                    )
            return side * PLACES + column, found

        def measure(n, m):
            cell, near = blocks(n)
            columns = jcols[packed(near[m][1])]
            put_distances(dist, m, rows_of(irows, cell), scales[0, near[m][0]], columns)

        def step(n, carry):
            cell, near = blocks(n)
            following = jnp.minimum(n + 1, 15)
            total = jnp.zeros((8, 128), F32)
            for m in range(6):
                total = add_density(total, dist, m, masses, near[m][1])
                measure(following, m)
            rhos[pl.ds(cell, 1), :] = density_of(total)
            return carry

        rhos[...] = jnp.zeros_like(rhos)
        for m in range(6):
            measure(0, m)
        lax.fori_loop(0, 16, step, 0)


def beside_kernel(run, left, right, *refs):
    fields, irows, jcols, masses, rhos, jrows, scales, dist = refs[-8:]

    @pl.when(run[0] == 1)
    def _():
        for row in range(2):
            for f in range(7):
                fields[row, f, 8:10, :] = left[row, f, 6:8, :]
                fields[row, f, 10:12, :] = right[row, f, 0:2, :]
        fill_scales(scales)
        build_tables(2, (1,), fields, irows, jcols, masses, jrows)

        def blocks(n):
            side, far = n // 2, n % 2
            outer, inner = jnp.where(far == 1, 8, -1), jnp.where(far == 1, 7, 0)
            found = []
            for direction, row in ((1, side), (2 - 2 * side, 1 - side)):
                for b in (-1, 0, 1):
                    at = row * PLACES + place_of(outer + b)
                    found.append((0, row_index(direction, b), at))
                at = row * PLACES + place_of(outer)
                found.append((1, row_index(direction, 2 * far - 1), at))
            cells = [side * PLACES + place_of(column) for column in (outer, inner)]
            return cells, found

        def measure(n, m):
            cells, near = blocks(n)
            which, index, at = near[m]
            table = rows_of(irows, cells[which])
            put_distances(dist, m, table, scales[0, index], jcols[packed(at)])

        def step(n, carry):
            cells, near = blocks(n)
            following = jnp.minimum(n + 1, 3)
            totals = [jnp.zeros((8, 128), F32)] * 2
            for m in range(8):
                which, _, at = near[m]
                totals[which] = add_density(totals[which], dist, m, masses, at)
                measure(following, m)
            rhos[pl.ds(cells[0], 1), :] = density_of(totals[0])
            rhos[pl.ds(cells[1], 1), :] = density_of(totals[1]) + rhos[pl.ds(cells[1], 1), :]
            return carry

        for m in range(8):
            measure(0, m)
        lax.fori_loop(0, 4, step, 0)


def late_kernel(
    info, jump_ref, far, same, fields, irows, jcols, masses, partial, density, accel,
    ghosts, ghost_irows, ghost_jcols, ghost_masses, jrows,
    scales, rhos, ghost_rhos, crows, ghost_crows, dist, sums, even_slopes, odd_slopes,
):
    odd, jump = info[0], jump_ref[0]

    ghosts[...] = jnp.zeros_like(ghosts)
    for piece, side in ((same, 1 - odd), (far, odd)):
        for f in range(NEAR):
            value = piece[f * COLS : (f + 1) * COLS, :]
            if piece is far and f == 3:
                value = value + jump
            ghosts[side, f, 0:8, :] = value[2:10]
            ghosts[side, f, 8:10, :] = value[0:2]
            ghosts[side, f, 10:12, :] = value[10:12]
        for n, f in enumerate((0, 1, 2, 6)):
            at = (NEAR + n) * COLS
            value = piece[at : at + COLS, :]
            ghosts[2 + side, f, 0:8, :] = value[2:10]
            ghosts[2 + side, f, 8:10, :] = value[0:2]
            ghosts[2 + side, f, 10:12, :] = value[10:12]
    fill_scales(scales)
    build_tables(4, (0, 1), ghosts, ghost_irows, ghost_jcols, ghost_masses, jrows)

    def blocks(n):
        side, column = n // 10, n % 10 - 1
        return side * PLACES + place_of(column), side, [
            (who, row_index(direction, b), row * PLACES + place_of(column + b))
            for who, direction, row in (
                ("far", 2 * side, side + 2),
                ("near", 1, side),
                ("own", 2 - 2 * side, side),
                ("mine", 2 * side, side),
            )
            for b in (-1, 0, 1)
        ]

    def measure(n, m):
        cell, _, near = blocks(n)
        who, index, at = near[m]
        table = rows_of(irows if who == "mine" else ghost_irows, cell)
        columns = (jcols if who == "own" else ghost_jcols)[packed(at)]
        put_distances(dist, m, table, scales[0, index], columns)

    def density_step(n, carry):
        cell, _, near = blocks(n)
        following = jnp.minimum(n + 1, 19)
        ghost_total = jnp.zeros((8, 128), F32)
        own_total = jnp.zeros((8, 128), F32)
        for m in range(12):
            who, _, at = near[m]
            which = masses if who == "own" else ghost_masses
            if who == "mine":
                own_total = add_density(own_total, dist, m, which, at)
            else:
                ghost_total = add_density(ghost_total, dist, m, which, at)
            measure(following, m)
        ghost_rhos[pl.ds(cell, 1), :] = density_of(ghost_total)
        rhos[pl.ds(cell, 1), :] = density_of(own_total) + partial[pl.ds(cell, 1), :]
        return carry

    rhos[...] = jnp.zeros_like(rhos)
    ghost_rhos[...] = jnp.zeros_like(ghost_rhos)
    for m in range(12):
        measure(0, m)
    lax.fori_loop(0, 20, density_step, 0)

    def coefficients(source, densities, target):
        def step(n, carry):
            row, half = n // 2, n % 2
            base = n * (8 * DEPTH)
            cells = pl.ds(pl.multiple_of(half * 8, 8), 8)
            mass = source[row, 6, cells, :]
            rho = densities[pl.ds(pl.multiple_of(n * 8, 8), 8), :]
            share = mass / jnp.where(mass > 0.0, rho, 1.0)
            terms = []
            for weight in (mass, share):
                terms.append(weight)
                for f in range(3):
                    high, low = parts_of(2.0 * source[row, f, cells, :] - 1.0, 2)
                    terms.append(weight * (high + low))
                terms.append(weight)
                terms.append(weight)
            for f in range(3, 6):
                terms.append(share * source[row, f, cells, :])
            terms.append(jnp.zeros((8, 128), F32))
            for t, term in enumerate(terms):
                high, low = parts_of(term, 2)
                target[pl.ds(base + t, 8, stride=DEPTH), :] = high
                target[pl.ds(base + 16 + t, 8, stride=DEPTH), :] = low
            return carry

        lax.fori_loop(0, 4, step, 0)

    coefficients(fields, rhos, crows)
    coefficients(ghosts, ghost_rhos, ghost_crows)

    def force_blocks(n):
        side, column = n // 8, n % 8
        return side * PLACES + column, [
            (ghost, row_index(direction, b), row * PLACES + place_of(column + b))
            for ghost, direction, row in (
                (True, 2 * side, side),
                (False, 1, side),
                (False, 2 - 2 * side, 1 - side),
            )
            for b in (-1, 0, 1)
        ]

    def force_measure(n, m):
        cell, near = force_blocks(n)
        ghost, index, at = near[m]
        columns = (ghost_jcols if ghost else jcols)[packed(at)]
        put_distances(dist, m, rows_of(irows, cell), scales[0, index], columns)

    def gather_sums(n, slopes):
        _, near = force_blocks(n)
        total = jnp.zeros((DEPTH, 256), F32)
        for m in range(9):
            ghost, index, at = near[m]
            table = rows_of(ghost_crows if ghost else crows, at)
            left_side = (table * scales[1, index]).astype(BF16)
            total = total + jnp.dot(
                jnp.concatenate([left_side, left_side], axis=1),
                slopes[256 * m : 256 * (m + 1), :],
                preferred_element_type=F32,
            )
        total = total[0:16] + total[16:32]
        for half in range(2):
            at = pl.ds(pl.multiple_of(n * 16, 16), 16)
            sums[half, at, :] = total[:, 128 * half : 128 * (half + 1)]

    def put_slopes(n, slopes):
        following = jnp.minimum(n + 1, 15)
        for m in range(9):
            for at in range(0, 128, 32):
                y = jnp.maximum(dist[m, at : at + 32, :], 1e-12)
                inverse = lax.rsqrt(y)
                q = y * inverse
                reach = jnp.maximum(2.0 - q, 0.0)
                slope = jnp.where(y < 1.0, 4.0 - 3.0 * q, reach * reach * inverse)
                soft = lax.rsqrt(y + 4.0 * SOFTENING)
                damped = slope * (y * (soft * soft))
                both = jnp.concatenate([slope, damped], axis=1)
                high = both.astype(BF16)
                base = 256 * m + at
                slopes[base : base + 32, :] = high
                slopes[base + 128 : base + 160, :] = (both - high.astype(F32)).astype(BF16)
            force_measure(following, m)

    def force_step(n, carry):
        gather_sums(jnp.maximum(2 * n - 1, 0), odd_slopes)
        put_slopes(2 * n, even_slopes)
        gather_sums(2 * n, even_slopes)
        put_slopes(2 * n + 1, odd_slopes)
        return carry

    for m in range(9):
        force_measure(0, m)
    lax.fori_loop(0, 8, force_step, 0)
    gather_sums(15, odd_slopes)

    for row in range(2):
        mass = fields[row, 6, 0:8, :]
        valid = mass > 0.0
        rho = rhos[row * PLACES : row * PLACES + 8, :]
        density[row] = jnp.where(valid, rho, 0.0)
        inverse_rho = 1.0 / jnp.where(valid, rho, 1.0)

        def term(k, half):
            return sums[half, pl.ds(row * 128 + k, 8, stride=16), :]

        mass_sum, share_sum, drag_sum = term(0, 0), term(6, 0), term(6, 1)
        pressure_scale = -3.0 * KERNEL_NORM * -SOUND_SQ * 0.5
        viscous_scale = -3.0 * KERNEL_NORM * 2.0 * VISCOSITY
        for f in range(3):
            high, low = parts_of(2.0 * fields[row, f, 0:8, :] - 1.0, 2)
            x = high + low
            first = x * mass_sum - term(1 + f, 0)
            second = x * share_sum - term(7 + f, 0)
            if f < 2:
                first = first - 2.0 * term(4 + f, 0)
                second = second - 2.0 * term(10 + f, 0)
            viscous = fields[row, 3 + f, 0:8, :] * drag_sum - term(12 + f, 1)
            value = pressure_scale * (first * inverse_rho + second)
            value = value + viscous_scale * viscous * inverse_rho
            accel[row, f] = jnp.where(valid, value, 0.0)


def scratch_of(tables, rows):
    return [
        pltpu.VMEM((t.shape[0] // 2 * rows, *t.shape[1:]), t.dtype) for t in tables
    ]


def params(mib):
    return pltpu.CompilerParams(vmem_limit_bytes=mib * 2**20)


def local(rows_axis, columns_axis, position, velocity, particle_mass, cell_counts, shear_shift):
    slabs, blocks = lax.axis_size(rows_axis), lax.axis_size(columns_axis)
    axes = (rows_axis, columns_axis)
    half = blocks // 2
    slab = lax.axis_index(rows_axis)
    past = shear_shift[0] - half * particle_mass.shape[1]

    slot = jnp.arange(particle_mass.shape[2], dtype=jnp.int32)
    weight = jnp.where(slot < cell_counts[:, :, None], particle_mass, 0.0)
    ring = [(i, (i + 1) % blocks) for i in range(blocks)]
    fields = jnp.concatenate(
        [
            jnp.transpose(position, (0, 3, 1, 2)),
            jnp.transpose(velocity, (0, 3, 1, 2)),
            weight[:, None],
        ],
        axis=1,
    )
    shapes = (*TABLES, jax.ShapeDtypeStruct((2 * PLACES, 128), F32))

    def tables_call(kernel, run, inputs, tables, blocks):
        count = len(inputs) + 1
        return pl.pallas_call(
            kernel,
            out_shape=shapes,
            in_specs=[SMEM] + [VMEM] * (len(inputs) + len(tables)),
            out_specs=[VMEM] * 5,
            scratch_shapes=[
                pltpu.VMEM((2 * PLACES * DEPTH, 128), F32),
                pltpu.VMEM((1, 9, DEPTH, 128), F32),
                pltpu.VMEM((blocks, 128, 128), F32),
            ],
            input_output_aliases={count + n: n for n in range(len(tables))},
            compiler_params=params(8),
            cost_estimate=pl.CostEstimate(
                flops=100_000_000, bytes_accessed=4_000_000, transcendentals=1_000_000
            ),
        )(run.astype(jnp.int32)[None], *inputs, *tables)

    block = lax.axis_index(columns_axis)
    edge = (slab == 0) | (slab == slabs - 1)
    own_now = [block <= 1, (block > 1) & ~(edge & (block >= half)), edge & (block >= half)]
    soon = edge & (block > 1) & (block < half)
    beside_now = [soon, ~edge, edge & ~soon]

    def own_work(which, tables):
        return tables_call(own_kernel, own_now[which], (fields,), tables, 6)

    def beside_work(which, tables):
        return tables_call(beside_kernel, beside_now[which], (left, right), tables, 8)

    left = lax.ppermute(fields, columns_axis, ring)
    tables = own_work(0, ())
    right = lax.ppermute(fields, columns_axis, [(j, i) for i, j in ring])
    tables = own_work(1, tables)

    odd = lax.rem(slab, 2)
    start = 6 + jnp.where(slab == slabs - 1, past, jnp.where(slab == 0, -past, 0))
    info = jnp.stack([odd, start]).astype(jnp.int32)
    sent = jax.ShapeDtypeStruct((SENT, 128), F32)
    far, same = pl.pallas_call(
        window_kernel,
        out_shape=(sent, sent),
        in_specs=[SMEM, VMEM, VMEM, VMEM],
        out_specs=(VMEM, VMEM),
        compiler_params=params(4),
        name="window",
    )(info, left, fields, right)

    same_pairs, far_pairs = [], []
    for s in range(slabs):
        for b in range(blocks):
            me = s * blocks + b
            same_pairs.append((me, (s + 1 if s % 2 == 0 else s - 1) * blocks + b))
            other, to = (s - 1, b) if s % 2 == 0 else (s + 1, b)
            if other < 0 or other >= slabs:
                other, to = other % slabs, (b + half) % blocks
            far_pairs.append((me, other * blocks + to))
    tables = beside_work(0, tables)
    far = lax.ppermute(far, axes, far_pairs)
    tables = beside_work(1, tables)
    same = lax.ppermute(same, axes, same_pairs)
    tables = own_work(2, tables)
    tables = beside_work(2, tables)

    jump = jnp.where(slab == slabs - 1, SHEAR_JUMP, jnp.where(slab == 0, -SHEAR_JUMP, 0.0))
    density, accel = pl.pallas_call(
        late_kernel,
        out_shape=(
            jax.ShapeDtypeStruct((2, 8, 128), F32),
            jax.ShapeDtypeStruct((2, 3, 8, 128), F32),
        ),
        in_specs=[SMEM, SMEM] + [VMEM] * 7,
        out_specs=(VMEM, VMEM),
        scratch_shapes=[
            *scratch_of(TABLES, 4),
            pltpu.VMEM((4 * PLACES * DEPTH, 128), F32),
            pltpu.VMEM((2, 9, DEPTH, 128), F32),
            pltpu.VMEM((2 * PLACES, 128), F32),
            pltpu.VMEM((2 * PLACES, 128), F32),
            pltpu.VMEM((2 * PLACES * DEPTH, 128), F32),
            pltpu.VMEM((2 * PLACES * DEPTH, 128), F32),
            pltpu.VMEM((12, 128, 128), F32),
            pltpu.VMEM((2, 16 * 16, 128), F32),
            pltpu.VMEM((9 * 256, 256), BF16),
            pltpu.VMEM((9 * 256, 256), BF16),
        ],
        compiler_params=params(24),
        name="late",
    )(info, jump.astype(F32)[None], far, same, *tables)
    return (density, jnp.transpose(accel, (0, 2, 3, 1)))


def solution(mesh):
    placed = (
        P("gy", "gx", None, None),
        P("gy", "gx", None, None),
        P("gy", "gx", None),
        P("gy", "gx"),
        P(),
    )

    def step(*args):
        return local("gy", "gx", *args)

    return jax.shard_map(
        step,
        mesh=mesh,
        in_specs=placed,
        out_specs=(P("gy", "gx", None), P("gy", "gx", None, None)),
        check_vma=False,
    )
```

```python
import math

import jax
import jax.numpy as jnp
from jax import lax
from jax.experimental import pallas as pl
from jax.experimental.pallas import tpu as pltpu
from jax.sharding import PartitionSpec as P


SMOOTHING = 0.5
KERNEL_NORM = 1.0 / (math.pi * SMOOTHING**3)
SOUND_SQ = 0.2
VISCOSITY = 0.05
SOFTENING = 0.0025
SHEAR_JUMP = 1.0

COLS, PLACES = 12, 16
DEPTH = 32
TERMS = 16
NEAR = 7
SENT = 136
BF16, F32 = jnp.bfloat16, jnp.float32
NEIGHBOURS = [(a, b) for a in (-1, 0, 1) for b in (-1, 0, 1)]
VMEM = pl.BlockSpec(memory_space=pltpu.VMEM)
SMEM = pl.BlockSpec(memory_space=pltpu.SMEM)
TABLES = (
    jax.ShapeDtypeStruct((2, 7, PLACES, 128), F32),
    jax.ShapeDtypeStruct((2 * PLACES * DEPTH, 128), F32),
    jax.ShapeDtypeStruct((2 * COLS, 128, DEPTH), BF16),
    jax.ShapeDtypeStruct((2 * COLS, 128, 128), F32),
)


def place_of(column):
    return column & (PLACES - 1)


def window_kernel(info, left, own, right, far_out, same_out):
    odd, start = info[0], info[1]
    for out in (far_out, same_out):
        near_row = jnp.where(odd == 1, 1, 0)
        if out is same_out:
            near_row = 1 - near_row
        place = 0
        for row, fields in ((near_row, range(NEAR)), (1 - near_row, (0, 1, 2, 6))):
            for f in fields:
                wide = jnp.concatenate([left[row, f], own[row, f], right[row, f]], axis=0)
                if out is same_out:
                    piece = wide[6:18]
                else:
                    piece = pltpu.roll(wide, 24 - start, 0)[0:COLS]
                out[place : place + COLS, :] = piece
                place += COLS
        out[place:SENT, :] = jnp.zeros((SENT - place, 128), F32)


def parts_of(x, count):
    parts = []
    for _ in range(count - 1):
        part = x.astype(BF16).astype(F32)
        parts.append(part)
        x = x - part
    parts.append(x.astype(BF16).astype(F32))
    return parts


def fill_scales(scales):
    k = lax.broadcasted_iota(jnp.int32, (DEPTH, 128), 0)
    for n, (a, b) in enumerate(NEIGHBOURS):
        scale = jnp.where(k < 18, 1.0, 0.0)
        scale = jnp.where((k >= 18) & (k < 22), float(b), scale)
        scale = jnp.where((k >= 22) & (k < 26), float(a), scale)
        scale = jnp.where(k == 26, float(a * a + b * b), scale)
        scales[0, n] = scale
        if scales.shape[0] > 1:
            scale = jnp.where((k == 4) | (k == 10) | (k == 20) | (k == 26), float(b), 1.0)
            scale = jnp.where((k == 5) | (k == 11) | (k == 21) | (k == 27), float(a), scale)
            scales[1, n] = scale


def build_tables(rows, halves, fields, irows, jcols, masses, jrows):
    k = lax.broadcasted_iota(jnp.int32, (DEPTH, 128), 0)
    ones_j = jnp.where(((k >= 15) & (k < 20)) | (k == 22) | (k == 23) | (k == 26), 1.0, 0.0)
    ones_i = jnp.where((k >= 12) & (k < 15), 1.0, 0.0)
    ones_i = jnp.where((k == 20) | (k == 21) | (k >= 24) & (k < 27), 4.0, ones_i)
    pick_mass = jnp.where((k >= 27) & (k < 30), 1.0, 0.0).astype(BF16)

    count = len(halves)

    def build(n, carry):
        row, half = n // count, n % count + halves[0]
        step = row * 2 + half
        base = pl.multiple_of(step * (8 * DEPTH), 8 * DEPTH)
        cells = pl.ds(pl.multiple_of(half * 8, 8), 8)
        for c in range(8):
            jrows[pl.ds(base + c * DEPTH, DEPTH), :] = ones_j
            irows[pl.ds(base + c * DEPTH, DEPTH), :] = ones_i

        def put(table, k, value):
            table[pl.ds(base + k, 8, stride=DEPTH), :] = value

        norm = jnp.zeros((8, 128), F32)
        for f in range(3):
            x = 2.0 * fields[row, f, cells, :] - 1.0
            high, low = parts_of(x, 2)
            both = high + low
            norm = norm + both * both
            for k, (mine, other) in enumerate(((high, high), (high, low), (low, high), (low, low))):
                put(jrows, 4 * f + k, mine)
                put(irows, 4 * f + k, -2.0 * other)
            if f < 2:
                at = 18 + 4 * f
                put(jrows, at + 2, high)
                put(jrows, at + 3, low)
                put(irows, at, -4.0 * high)
                put(irows, at + 1, -4.0 * low)
        for k, part in enumerate(parts_of(norm, 3)):
            put(jrows, 12 + k, part)
            put(irows, 15 + k, part)
        for k, part in enumerate(parts_of(fields[row, 6, cells, :], 3)):
            put(jrows, 27 + k, part)
        return carry

    lax.fori_loop(0, rows * count, build, 0)

    def turn_row(row, carry):
        for column in range(-2, 10):
            if (0 if 0 <= column < 8 else 1) not in halves:
                continue
            c = column + 2
            cell = row * PLACES + place_of(column)
            table = jrows[pl.ds(pl.multiple_of(cell * DEPTH, DEPTH), DEPTH), :]
            flipped = table.T.astype(BF16)
            jcols[row * COLS + c] = flipped
            masses[row * COLS + c] = jnp.dot(flipped, pick_mass, preferred_element_type=F32)
        return carry

    lax.fori_loop(0, rows, turn_row, 0)


def rows_of(table, cell):
    return table[pl.ds(pl.multiple_of(cell * DEPTH, DEPTH), DEPTH), :]


def put_distances(dist, m, table, scale, columns):
    right_side = (table * scale).astype(BF16)
    dist[m] = jnp.dot(columns, right_side, preferred_element_type=F32)


def add_density(total, dist, m, masses, cell):
    for at in range(0, 128, 32):
        y = jnp.maximum(dist[m, at : at + 32, :], 1e-12)
        q = y * lax.rsqrt(y)
        reach = jnp.maximum(2.0 - q, 0.0)
        inner = 4.0 - 3.0 * y * reach
        outer = reach * reach * reach
        w = jnp.where(y < 1.0, inner, outer) * masses[cell, at : at + 32, :]
        total = total + ((w[0:8] + w[8:16]) + (w[16:24] + w[24:32]))
    return total


def density_of(total):
    return jnp.sum(total, axis=0, keepdims=True) * (0.25 * KERNEL_NORM)


def row_index(direction, b):
    return direction * 3 + b + 1


def own_kernel(run, own, *refs):
    fields, irows, jcols, masses, rhos, jrows, scales, dist = refs[-8:]

    @pl.when(run[0] == 1)
    def _():
        fields[...] = jnp.zeros_like(fields)
        for row in range(2):
            for f in range(7):
                fields[row, f, 0:8, :] = own[row, f]
        fill_scales(scales)
        build_tables(2, (0,), fields, irows, jcols, masses, jrows)
        for at in (1, 10, COLS + 1, COLS + 10):
            jcols[at] = jnp.zeros((128, DEPTH), BF16)
            masses[at] = jnp.zeros((128, 128), F32)

        def blocks(n):
            side, column = n // 8, n % 8
            found = [
                (row_index(direction, b), row * COLS + column + (b + 2))
                for direction, row in ((1, side), (2 - 2 * side, 1 - side))
                for b in (-1, 0, 1)
            ]
            return side * PLACES + column, found

        def measure(n, m):
            cell, near = blocks(n)
            columns = jcols[near[m][1]]
            put_distances(dist, m, rows_of(irows, cell), scales[0, near[m][0]], columns)

        def step(n, carry):
            cell, near = blocks(n)
            following = jnp.minimum(n + 1, 15)
            total = jnp.zeros((8, 128), F32)
            for m in range(6):
                total = add_density(total, dist, m, masses, near[m][1])
                measure(following, m)
            rhos[pl.ds(cell, 1), :] = density_of(total)
            return carry

        rhos[...] = jnp.zeros_like(rhos)
        for m in range(6):
            measure(0, m)
        lax.fori_loop(0, 16, step, 0)


def beside_kernel(run, left, right, *refs):
    fields, irows, jcols, masses, rhos, jrows, scales, dist = refs[-8:]

    @pl.when(run[0] == 1)
    def _():
        for row in range(2):
            for f in range(7):
                fields[row, f, 8:10, :] = right[row, f, 0:2, :]
                fields[row, f, 14:16, :] = left[row, f, 6:8, :]
        fill_scales(scales)
        build_tables(2, (1,), fields, irows, jcols, masses, jrows)

        def blocks(n):
            side, far = n // 2, n % 2
            outer, inner = jnp.where(far == 1, 8, -1), jnp.where(far == 1, 7, 0)
            found = []
            for direction, row in ((1, side), (2 - 2 * side, 1 - side)):
                for b in (-1, 0, 1):
                    found.append((0, row_index(direction, b), row * COLS + outer + (b + 2)))
                at = row * COLS + outer + 2
                found.append((1, row_index(direction, 2 * far - 1), at))
            cells = [side * PLACES + place_of(column) for column in (outer, inner)]
            return cells, found

        def measure(n, m):
            cells, near = blocks(n)
            which, index, at = near[m]
            table = rows_of(irows, cells[which])
            put_distances(dist, m, table, scales[0, index], jcols[at])

        def step(n, carry):
            cells, near = blocks(n)
            following = jnp.minimum(n + 1, 3)
            totals = [jnp.zeros((8, 128), F32)] * 2
            for m in range(8):
                which, _, at = near[m]
                totals[which] = add_density(totals[which], dist, m, masses, at)
                measure(following, m)
            rhos[pl.ds(cells[0], 1), :] = density_of(totals[0])
            rhos[pl.ds(cells[1], 1), :] = density_of(totals[1]) + rhos[pl.ds(cells[1], 1), :]
            return carry

        for m in range(8):
            measure(0, m)
        lax.fori_loop(0, 4, step, 0)


def late_kernel(
    info, jump_ref, far, same, fields, irows, jcols, masses, partial, density, accel,
    ghosts, ghost_irows, ghost_jcols, ghost_masses, jrows,
    scales, rhos, ghost_rhos, crows, ghost_crows, dist, sums, even_slopes, odd_slopes,
):
    odd, jump = info[0], jump_ref[0]

    ghosts[...] = jnp.zeros_like(ghosts)
    for piece, side in ((same, 1 - odd), (far, odd)):
        for f in range(NEAR):
            value = piece[f * COLS : (f + 1) * COLS, :]
            if piece is far and f == 3:
                value = value + jump
            ghosts[side, f, 0:8, :] = value[2:10]
            ghosts[side, f, 8:10, :] = value[10:12]
            ghosts[side, f, 14:16, :] = value[0:2]
        for n, f in enumerate((0, 1, 2, 6)):
            at = (NEAR + n) * COLS
            value = piece[at : at + COLS, :]
            ghosts[2 + side, f, 0:8, :] = value[2:10]
            ghosts[2 + side, f, 8:10, :] = value[10:12]
            ghosts[2 + side, f, 14:16, :] = value[0:2]
    fill_scales(scales)
    build_tables(4, (0, 1), ghosts, ghost_irows, ghost_jcols, ghost_masses, jrows)

    def blocks(n):
        side, column = n // 10, n % 10 - 1
        return side * PLACES + place_of(column), side, [
            (who, row_index(direction, b), row * COLS + column + (b + 2))
            for who, direction, row in (
                ("far", 2 * side, side + 2),
                ("near", 1, side),
                ("own", 2 - 2 * side, side),
                ("mine", 2 * side, side),
            )
            for b in (-1, 0, 1)
        ]

    def measure(n, m):
        cell, _, near = blocks(n)
        who, index, at = near[m]
        table = rows_of(irows if who == "mine" else ghost_irows, cell)
        columns = (jcols if who == "own" else ghost_jcols)[at]
        put_distances(dist, m, table, scales[0, index], columns)

    def density_step(n, carry):
        cell, _, near = blocks(n)
        following = jnp.minimum(n + 1, 19)
        ghost_total = jnp.zeros((8, 128), F32)
        own_total = jnp.zeros((8, 128), F32)
        for m in range(12):
            who, _, at = near[m]
            which = masses if who == "own" else ghost_masses
            if who == "mine":
                own_total = add_density(own_total, dist, m, which, at)
            else:
                ghost_total = add_density(ghost_total, dist, m, which, at)
            measure(following, m)
        ghost_rhos[pl.ds(cell, 1), :] = density_of(ghost_total)
        rhos[pl.ds(cell, 1), :] = density_of(own_total) + partial[pl.ds(cell, 1), :]
        return carry

    rhos[...] = jnp.zeros_like(rhos)
    ghost_rhos[...] = jnp.zeros_like(ghost_rhos)
    for m in range(12):
        measure(0, m)
    lax.fori_loop(0, 20, density_step, 0)

    def coefficients(source, densities, target):
        def step(n, carry):
            row, half = n // 2, n % 2
            base = n * (8 * TERMS)
            cells = pl.ds(pl.multiple_of(half * 8, 8), 8)
            mass = source[row, 6, cells, :]
            rho = densities[pl.ds(pl.multiple_of(n * 8, 8), 8), :]
            share = mass / jnp.where(mass > 0.0, rho, 1.0)
            terms = []
            for weight in (mass, share):
                terms.append(weight)
                for f in range(3):
                    high, low = parts_of(2.0 * source[row, f, cells, :] - 1.0, 2)
                    terms.append(weight * (high + low))
                terms.append(weight)
                terms.append(weight)
            for f in range(3, 6):
                terms.append(share * source[row, f, cells, :])
            terms.append(jnp.zeros((8, 128), F32))
            for t, term in enumerate(terms):
                target[pl.ds(base + t, 8, stride=TERMS), :] = term
            return carry

        lax.fori_loop(0, 4, step, 0)

    coefficients(fields, rhos, crows)
    coefficients(ghosts, ghost_rhos, ghost_crows)

    def force_blocks(n):
        side, column = n // 8, n % 8
        return side * PLACES + column, [
            (ghost, row_index(direction, b), row, column + b)
            for ghost, direction, row in (
                (True, 2 * side, side),
                (False, 1, side),
                (False, 2 - 2 * side, 1 - side),
            )
            for b in (-1, 0, 1)
        ]

    def force_measure(n, m):
        cell, near = force_blocks(n)
        ghost, index, row, column = near[m]
        columns = (ghost_jcols if ghost else jcols)[row * COLS + column + 2]
        put_distances(dist, m, rows_of(irows, cell), scales[0, index], columns)

    def gather_sums(n, slopes):
        _, near = force_blocks(n)
        total = jnp.zeros((DEPTH, 256), F32)
        for m in range(9):
            ghost, index, row, column = near[m]
            at = row * PLACES + place_of(column)
            table = ghost_crows if ghost else crows
            table = table[pl.ds(pl.multiple_of(at * TERMS, TERMS), TERMS), :]
            left_side = jnp.concatenate(parts_of(table * scales[1, index, 0:TERMS, :], 2), axis=0)
            left_side = left_side.astype(BF16)
            total = total + jnp.dot(
                jnp.concatenate([left_side, left_side], axis=1),
                slopes[256 * m : 256 * (m + 1), :],
                preferred_element_type=F32,
            )
        total = total[0:16] + total[16:32]
        for half in range(2):
            at = pl.ds(pl.multiple_of(n * 16, 16), 16)
            sums[half, at, :] = total[:, 128 * half : 128 * (half + 1)]

    def put_slopes(n, slopes):
        following = jnp.minimum(n + 1, 15)
        for m in range(9):
            for at in range(0, 128, 32):
                y = jnp.maximum(dist[m, at : at + 32, :], 1e-12)
                inverse = lax.rsqrt(y)
                q = y * inverse
                reach = jnp.maximum(2.0 - q, 0.0)
                slope = jnp.where(y < 1.0, 4.0 - 3.0 * q, reach * reach * inverse)
                soft = lax.rsqrt(y + 4.0 * SOFTENING)
                damped = slope * (y * (soft * soft))
                both = jnp.concatenate([slope, damped], axis=1)
                high = both.astype(BF16)
                base = 256 * m + at
                slopes[base : base + 32, :] = high
                slopes[base + 128 : base + 160, :] = (both - high.astype(F32)).astype(BF16)
            force_measure(following, m)

    def force_step(n, carry):
        gather_sums(jnp.maximum(2 * n - 1, 0), odd_slopes)
        put_slopes(2 * n, even_slopes)
        gather_sums(2 * n, even_slopes)
        put_slopes(2 * n + 1, odd_slopes)
        return carry

    for m in range(9):
        force_measure(0, m)
    lax.fori_loop(0, 8, force_step, 0)
    gather_sums(15, odd_slopes)

    for row in range(2):
        mass = fields[row, 6, 0:8, :]
        valid = mass > 0.0
        rho = rhos[row * PLACES : row * PLACES + 8, :]
        density[row] = jnp.where(valid, rho, 0.0)
        inverse_rho = 1.0 / jnp.where(valid, rho, 1.0)

        def term(k, half):
            return sums[half, pl.ds(row * 128 + k, 8, stride=16), :]

        mass_sum, share_sum, drag_sum = term(0, 0), term(6, 0), term(6, 1)
        pressure_scale = -3.0 * KERNEL_NORM * -SOUND_SQ * 0.5
        viscous_scale = -3.0 * KERNEL_NORM * 2.0 * VISCOSITY
        for f in range(3):
            high, low = parts_of(2.0 * fields[row, f, 0:8, :] - 1.0, 2)
            x = high + low
            first = x * mass_sum - term(1 + f, 0)
            second = x * share_sum - term(7 + f, 0)
            if f < 2:
                first = first - 2.0 * term(4 + f, 0)
                second = second - 2.0 * term(10 + f, 0)
            viscous = fields[row, 3 + f, 0:8, :] * drag_sum - term(12 + f, 1)
            value = pressure_scale * (first * inverse_rho + second)
            value = value + viscous_scale * viscous * inverse_rho
            accel[row, f] = jnp.where(valid, value, 0.0)


def scratch_of(tables, rows):
    return [
        pltpu.VMEM((t.shape[0] // 2 * rows, *t.shape[1:]), t.dtype) for t in tables
    ]


def params(mib):
    return pltpu.CompilerParams(vmem_limit_bytes=mib * 2**20)


def local(rows_axis, columns_axis, position, velocity, particle_mass, cell_counts, shear_shift):
    slabs, blocks = lax.axis_size(rows_axis), lax.axis_size(columns_axis)
    axes = (rows_axis, columns_axis)
    half = blocks // 2
    slab = lax.axis_index(rows_axis)
    past = shear_shift[0] - half * particle_mass.shape[1]

    ring = [(i, (i + 1) % blocks) for i in range(blocks)]
    fields = jnp.concatenate(
        [
            jnp.transpose(position, (0, 3, 1, 2)),
            jnp.transpose(velocity, (0, 3, 1, 2)),
            particle_mass[:, None],
        ],
        axis=1,
    )
    field = lax.broadcasted_iota(jnp.int32, fields.shape, 1)
    slot = lax.broadcasted_iota(jnp.int32, fields.shape, 3)
    fields = jnp.where((field < 6) | (slot < cell_counts[:, None, :, None]), fields, 0.0)
    shapes = (*TABLES, jax.ShapeDtypeStruct((2 * PLACES, 128), F32))

    def tables_call(kernel, run, inputs, tables, blocks):
        count = len(inputs) + 1
        return pl.pallas_call(
            kernel,
            out_shape=shapes,
            in_specs=[SMEM] + [VMEM] * (len(inputs) + len(tables)),
            out_specs=[VMEM] * 5,
            scratch_shapes=[
                pltpu.VMEM((2 * PLACES * DEPTH, 128), F32),
                pltpu.VMEM((1, 9, DEPTH, 128), F32),
                pltpu.VMEM((blocks, 128, 128), F32),
            ],
            input_output_aliases={count + n: n for n in range(len(tables))},
            compiler_params=params(8),
            cost_estimate=pl.CostEstimate(
                flops=100_000_000, bytes_accessed=4_000_000, transcendentals=1_000_000
            ),
        )(run.astype(jnp.int32)[None], *inputs, *tables)

    block = lax.axis_index(columns_axis)
    edge = (slab == 0) | (slab == slabs - 1)
    corner = (block == 0) & (slab == 0)
    ahead, late = (block == 0) & ~corner, edge & (block >= half) | corner
    own_now = [ahead, ~(ahead | late), late]

    def own_work(which, tables):
        return tables_call(own_kernel, own_now[which], (fields,), tables, 6)

    left = lax.ppermute(fields, columns_axis, ring)
    tables = own_work(0, ())
    right = lax.ppermute(fields, columns_axis, [(j, i) for i, j in ring])
    tables = own_work(1, tables)

    odd = lax.rem(slab, 2)
    start = 6 + jnp.where(slab == slabs - 1, past, jnp.where(slab == 0, -past, 0))
    info = jnp.stack([odd, start]).astype(jnp.int32)
    sent = jax.ShapeDtypeStruct((SENT, 128), F32)
    far, same = pl.pallas_call(
        window_kernel,
        out_shape=(sent, sent),
        in_specs=[SMEM, VMEM, VMEM, VMEM],
        out_specs=(VMEM, VMEM),
        compiler_params=params(4),
        name="window",
    )(info, left, fields, right)

    same_pairs, far_pairs = [], []
    for s in range(slabs):
        for b in range(blocks):
            me = s * blocks + b
            same_pairs.append((me, (s + 1 if s % 2 == 0 else s - 1) * blocks + b))
            other, to = (s - 1, b) if s % 2 == 0 else (s + 1, b)
            if other < 0 or other >= slabs:
                other, to = other % slabs, (b + half) % blocks
            far_pairs.append((me, other * blocks + to))
    far = lax.ppermute(far, axes, far_pairs)
    tables = own_work(2, tables)
    tables = tables_call(beside_kernel, block >= 0, (left, right), tables, 8)
    same = lax.ppermute(same, axes, same_pairs)

    jump = jnp.where(slab == slabs - 1, SHEAR_JUMP, jnp.where(slab == 0, -SHEAR_JUMP, 0.0))
    density, accel = pl.pallas_call(
        late_kernel,
        out_shape=(
            jax.ShapeDtypeStruct((2, 8, 128), F32),
            jax.ShapeDtypeStruct((2, 3, 8, 128), F32),
        ),
        in_specs=[SMEM, SMEM] + [VMEM] * 7,
        out_specs=(VMEM, VMEM),
        scratch_shapes=[
            *scratch_of(TABLES, 4),
            pltpu.VMEM((4 * PLACES * DEPTH, 128), F32),
            pltpu.VMEM((2, 9, DEPTH, 128), F32),
            pltpu.VMEM((2 * PLACES, 128), F32),
            pltpu.VMEM((2 * PLACES, 128), F32),
            pltpu.VMEM((2 * PLACES * TERMS, 128), F32),
            pltpu.VMEM((2 * PLACES * TERMS, 128), F32),
            pltpu.VMEM((12, 128, 128), F32),
            pltpu.VMEM((2, 16 * 16, 128), F32),
            pltpu.VMEM((9 * 256, 256), BF16),
            pltpu.VMEM((9 * 256, 256), BF16),
        ],
        compiler_params=params(24),
        name="late",
    )(info, jump.astype(F32)[None], far, same, *tables)
    return (density, jnp.transpose(accel, (0, 2, 3, 1)))


def solution(mesh):
    placed = (
        P("gy", "gx", None, None),
        P("gy", "gx", None, None),
        P("gy", "gx", None),
        P("gy", "gx"),
        P(),
    )

    def step(*args):
        return local("gy", "gx", *args)

    return jax.shard_map(
        step,
        mesh=mesh,
        in_specs=placed,
        out_specs=(P("gy", "gx", None), P("gy", "gx", None, None)),
        check_vma=False,
    )
```

```python
import math

import jax
import jax.numpy as jnp
from jax import lax
from jax.experimental import pallas as pl
from jax.experimental.pallas import tpu as pltpu
from jax.sharding import PartitionSpec as P


SMOOTHING = 0.5
KERNEL_NORM = 1.0 / (math.pi * SMOOTHING**3)
SOUND_SQ = 0.2
VISCOSITY = 0.05
SOFTENING = 0.0025
SHEAR_JUMP = 1.0

COLS, PLACES = 12, 16
DEPTH = 32
TERMS = 16
NEAR = 7
SENT = 136
BF16, F32 = jnp.bfloat16, jnp.float32
NEIGHBOURS = [(a, b) for a in (-1, 0, 1) for b in (-1, 0, 1)]
VMEM = pl.BlockSpec(memory_space=pltpu.VMEM)
SMEM = pl.BlockSpec(memory_space=pltpu.SMEM)
TABLES = (
    jax.ShapeDtypeStruct((2, 7, PLACES, 128), F32),
    jax.ShapeDtypeStruct((2 * PLACES * DEPTH, 128), F32),
    jax.ShapeDtypeStruct((2 * COLS, 128, DEPTH), BF16),
    jax.ShapeDtypeStruct((2 * COLS, 128, 128), F32),
)


def place_of(column):
    return column & (PLACES - 1)


def window_kernel(info, left, own, right, far_out, same_out):
    odd, start = info[0], info[1]
    for out in (far_out, same_out):
        near_row = jnp.where(odd == 1, 1, 0)
        if out is same_out:
            near_row = 1 - near_row
        place = 0
        for row, fields in ((near_row, range(NEAR)), (1 - near_row, (0, 1, 2, 6))):
            for f in fields:
                wide = jnp.concatenate([left[row, f], own[row, f], right[row, f]], axis=0)
                if out is same_out:
                    piece = wide[6:18]
                else:
                    piece = pltpu.roll(wide, 24 - start, 0)[0:COLS]
                out[place : place + COLS, :] = piece
                place += COLS
        out[place:SENT, :] = jnp.zeros((SENT - place, 128), F32)


def parts_of(x, count):
    parts = []
    for _ in range(count - 1):
        part = x.astype(BF16).astype(F32)
        parts.append(part)
        x = x - part
    parts.append(x.astype(BF16).astype(F32))
    return parts


def fill_scales(scales):
    k = lax.broadcasted_iota(jnp.int32, (DEPTH, 128), 0)
    for n, (a, b) in enumerate(NEIGHBOURS):
        scale = jnp.where(k < 18, 1.0, 0.0)
        scale = jnp.where((k >= 18) & (k < 22), float(b), scale)
        scale = jnp.where((k >= 22) & (k < 26), float(a), scale)
        scale = jnp.where(k == 26, float(a * a + b * b), scale)
        scales[0, n] = scale
        if scales.shape[0] > 1:
            scale = jnp.where((k == 4) | (k == 10) | (k == 20) | (k == 26), float(b), 1.0)
            scale = jnp.where((k == 5) | (k == 11) | (k == 21) | (k == 27), float(a), scale)
            scales[1, n] = scale


def build_tables(rows, halves, fields, irows, jcols, masses, jrows):
    k = lax.broadcasted_iota(jnp.int32, (DEPTH, 128), 0)
    ones_j = jnp.where(((k >= 15) & (k < 20)) | (k == 22) | (k == 23) | (k == 26), 1.0, 0.0)
    ones_i = jnp.where((k >= 12) & (k < 15), 1.0, 0.0)
    ones_i = jnp.where((k == 20) | (k == 21) | (k >= 24) & (k < 27), 4.0, ones_i)
    pick_mass = jnp.where((k >= 27) & (k < 30), 1.0, 0.0).astype(BF16)

    count = len(halves)

    def build(n, carry):
        row, half = n // count, n % count + halves[0]
        step = row * 2 + half
        base = pl.multiple_of(step * (8 * DEPTH), 8 * DEPTH)
        cells = pl.ds(pl.multiple_of(half * 8, 8), 8)
        for c in range(8):
            jrows[pl.ds(base + c * DEPTH, DEPTH), :] = ones_j
            irows[pl.ds(base + c * DEPTH, DEPTH), :] = ones_i

        def put(table, k, value):
            table[pl.ds(base + k, 8, stride=DEPTH), :] = value

        norm = jnp.zeros((8, 128), F32)
        for f in range(3):
            x = 2.0 * fields[row, f, cells, :] - 1.0
            high, low = parts_of(x, 2)
            both = high + low
            norm = norm + both * both
            for k, (mine, other) in enumerate(((high, high), (high, low), (low, high), (low, low))):
                put(jrows, 4 * f + k, mine)
                put(irows, 4 * f + k, -2.0 * other)
            if f < 2:
                at = 18 + 4 * f
                put(jrows, at + 2, high)
                put(jrows, at + 3, low)
                put(irows, at, -4.0 * high)
                put(irows, at + 1, -4.0 * low)
        for k, part in enumerate(parts_of(norm, 3)):
            put(jrows, 12 + k, part)
            put(irows, 15 + k, part)
        for k, part in enumerate(parts_of(fields[row, 6, cells, :], 3)):
            put(jrows, 27 + k, part)
        return carry

    lax.fori_loop(0, rows * count, build, 0)

    def turn_rows(pair, carry):
        for n in range(48):
            row, column = 2 * pair + n % 2, n // 2 - 2
            if column > 9 or (0 if 0 <= column < 8 else 1) not in halves:
                continue
            c = column + 2
            cell = row * PLACES + place_of(column)
            table = jrows[pl.ds(pl.multiple_of(cell * DEPTH, DEPTH), DEPTH), :]
            flipped = table.T.astype(BF16)
            jcols[row * COLS + c] = flipped
            masses[row * COLS + c] = jnp.dot(flipped, pick_mass, preferred_element_type=F32)
        return carry

    lax.fori_loop(0, rows // 2, turn_rows, 0)


def rows_of(table, cell):
    return table[pl.ds(pl.multiple_of(cell * DEPTH, DEPTH), DEPTH), :]


def put_distances(dist, m, table, scale, columns):
    right_side = (table * scale).astype(BF16)
    dist[m] = jnp.dot(columns, right_side, preferred_element_type=F32)


def add_density(total, dist, m, masses, cell):
    for at in range(0, 128, 32):
        y = jnp.maximum(dist[m, at : at + 32, :], 1e-12)
        q = y * lax.rsqrt(y)
        reach = jnp.maximum(2.0 - q, 0.0)
        inner = 4.0 - 3.0 * y * reach
        outer = reach * reach * reach
        w = jnp.where(y < 1.0, inner, outer) * masses[cell, at : at + 32, :]
        total = total + ((w[0:8] + w[8:16]) + (w[16:24] + w[24:32]))
    return total


def density_of(total):
    return jnp.sum(total, axis=0, keepdims=True) * (0.25 * KERNEL_NORM)


def row_index(direction, b):
    return direction * 3 + b + 1


def own_kernel(run, own, *refs):
    fields, irows, jcols, masses, rhos, jrows, scales, dist = refs[-8:]

    @pl.when(run[0] == 1)
    def _():
        fields[...] = jnp.zeros_like(fields)
        for row in range(2):
            for f in range(7):
                fields[row, f, 0:8, :] = own[row, f]
        fill_scales(scales)
        build_tables(2, (0,), fields, irows, jcols, masses, jrows)
        for at in (1, 10, COLS + 1, COLS + 10):
            jcols[at] = jnp.zeros((128, DEPTH), BF16)
            masses[at] = jnp.zeros((128, 128), F32)

        def blocks(n):
            side, column = n // 8, n % 8
            found = [
                (row_index(direction, b), row * COLS + column + (b + 2))
                for direction, row in ((1, side), (2 - 2 * side, 1 - side))
                for b in (-1, 0, 1)
            ]
            return side * PLACES + column, found

        def measure(n, m):
            cell, near = blocks(n)
            columns = jcols[near[m][1]]
            put_distances(dist, m, rows_of(irows, cell), scales[0, near[m][0]], columns)

        def step(n, carry):
            cell, near = blocks(n)
            following = jnp.minimum(n + 1, 15)
            total = jnp.zeros((8, 128), F32)
            for m in range(6):
                total = add_density(total, dist, m, masses, near[m][1])
                measure(following, m)
            rhos[pl.ds(cell, 1), :] = density_of(total)
            return carry

        rhos[...] = jnp.zeros_like(rhos)
        for m in range(6):
            measure(0, m)
        lax.fori_loop(0, 16, step, 0)


def beside_kernel(run, left, right, *refs):
    fields, irows, jcols, masses, rhos, jrows, scales, dist = refs[-8:]

    @pl.when(run[0] == 1)
    def _():
        for row in range(2):
            for f in range(7):
                fields[row, f, 8:10, :] = right[row, f, 0:2, :]
                fields[row, f, 14:16, :] = left[row, f, 6:8, :]
        fill_scales(scales)
        build_tables(2, (1,), fields, irows, jcols, masses, jrows)

        def blocks(n):
            side, far = n // 2, n % 2
            outer, inner = jnp.where(far == 1, 8, -1), jnp.where(far == 1, 7, 0)
            found = []
            for direction, row in ((1, side), (2 - 2 * side, 1 - side)):
                for b in (-1, 0, 1):
                    found.append((0, row_index(direction, b), row * COLS + outer + (b + 2)))
                at = row * COLS + outer + 2
                found.append((1, row_index(direction, 2 * far - 1), at))
            cells = [side * PLACES + place_of(column) for column in (outer, inner)]
            return cells, found

        def measure(n, m):
            cells, near = blocks(n)
            which, index, at = near[m]
            table = rows_of(irows, cells[which])
            put_distances(dist, m, table, scales[0, index], jcols[at])

        def step(n, carry):
            cells, near = blocks(n)
            following = jnp.minimum(n + 1, 3)
            totals = [jnp.zeros((8, 128), F32)] * 2
            for m in range(8):
                which, _, at = near[m]
                totals[which] = add_density(totals[which], dist, m, masses, at)
                measure(following, m)
            rhos[pl.ds(cells[0], 1), :] = density_of(totals[0])
            rhos[pl.ds(cells[1], 1), :] = density_of(totals[1]) + rhos[pl.ds(cells[1], 1), :]
            return carry

        for m in range(8):
            measure(0, m)
        lax.fori_loop(0, 4, step, 0)


def late_kernel(
    info, jump_ref, far, same, fields, irows, jcols, masses, partial, density, accel,
    ghosts, ghost_irows, ghost_jcols, ghost_masses, jrows,
    scales, rhos, ghost_rhos, crows, ghost_crows, dist, sums, even_slopes, odd_slopes,
):
    odd, jump = info[0], jump_ref[0]

    ghosts[...] = jnp.zeros_like(ghosts)
    for piece, side in ((same, 1 - odd), (far, odd)):
        for f in range(NEAR):
            value = piece[f * COLS : (f + 1) * COLS, :]
            if piece is far and f == 3:
                value = value + jump
            ghosts[side, f, 0:8, :] = value[2:10]
            ghosts[side, f, 8:10, :] = value[10:12]
            ghosts[side, f, 14:16, :] = value[0:2]
        for n, f in enumerate((0, 1, 2, 6)):
            at = (NEAR + n) * COLS
            value = piece[at : at + COLS, :]
            ghosts[2 + side, f, 0:8, :] = value[2:10]
            ghosts[2 + side, f, 8:10, :] = value[10:12]
            ghosts[2 + side, f, 14:16, :] = value[0:2]
    fill_scales(scales)
    build_tables(4, (0, 1), ghosts, ghost_irows, ghost_jcols, ghost_masses, jrows)

    def blocks(n):
        side, column = n // 10, n % 10 - 1
        return side * PLACES + place_of(column), side, [
            (who, row_index(direction, b), row * COLS + column + (b + 2))
            for who, direction, row in (
                ("far", 2 * side, side + 2),
                ("near", 1, side),
                ("own", 2 - 2 * side, side),
                ("mine", 2 * side, side),
            )
            for b in (-1, 0, 1)
        ]

    def measure(n, m):
        cell, _, near = blocks(n)
        who, index, at = near[m]
        table = rows_of(irows if who == "mine" else ghost_irows, cell)
        columns = (jcols if who == "own" else ghost_jcols)[at]
        put_distances(dist, m, table, scales[0, index], columns)

    def density_step(n, carry):
        cell, _, near = blocks(n)
        following = jnp.minimum(n + 1, 19)
        ghost_total = jnp.zeros((8, 128), F32)
        own_total = jnp.zeros((8, 128), F32)
        for m in range(12):
            who, _, at = near[m]
            which = masses if who == "own" else ghost_masses
            if who == "mine":
                own_total = add_density(own_total, dist, m, which, at)
            else:
                ghost_total = add_density(ghost_total, dist, m, which, at)
            measure(following, m)
        ghost_rhos[pl.ds(cell, 1), :] = density_of(ghost_total)
        rhos[pl.ds(cell, 1), :] = density_of(own_total) + partial[pl.ds(cell, 1), :]
        return carry

    rhos[...] = jnp.zeros_like(rhos)
    ghost_rhos[...] = jnp.zeros_like(ghost_rhos)
    for m in range(12):
        measure(0, m)
    lax.fori_loop(0, 20, density_step, 0)

    def coefficients(source, densities, target):
        def step(n, carry):
            row, half = n // 2, n % 2
            base = n * (8 * TERMS)
            cells = pl.ds(pl.multiple_of(half * 8, 8), 8)
            mass = source[row, 6, cells, :]
            rho = densities[pl.ds(pl.multiple_of(n * 8, 8), 8), :]
            share = mass / jnp.where(mass > 0.0, rho, 1.0)
            terms = []
            for weight in (mass, share):
                terms.append(weight)
                for f in range(3):
                    high, low = parts_of(2.0 * source[row, f, cells, :] - 1.0, 2)
                    terms.append(weight * (high + low))
                terms.append(weight)
                terms.append(weight)
            for f in range(3, 6):
                terms.append(share * source[row, f, cells, :])
            terms.append(jnp.zeros((8, 128), F32))
            for t, term in enumerate(terms):
                target[pl.ds(base + t, 8, stride=TERMS), :] = term
            return carry

        lax.fori_loop(0, 4, step, 0)

    coefficients(fields, rhos, crows)
    coefficients(ghosts, ghost_rhos, ghost_crows)

    def force_blocks(n):
        side, column = n // 8, n % 8
        return side * PLACES + column, [
            (ghost, row_index(direction, b), row, column + b)
            for ghost, direction, row in (
                (True, 2 * side, side),
                (False, 1, side),
                (False, 2 - 2 * side, 1 - side),
            )
            for b in (-1, 0, 1)
        ]

    def force_measure(n, m):
        cell, near = force_blocks(n)
        ghost, index, row, column = near[m]
        columns = (ghost_jcols if ghost else jcols)[row * COLS + column + 2]
        put_distances(dist, m, rows_of(irows, cell), scales[0, index], columns)

    def gather_sums(n, slopes):
        _, near = force_blocks(n)
        total = jnp.zeros((DEPTH, 256), F32)
        for m in range(9):
            ghost, index, row, column = near[m]
            at = row * PLACES + place_of(column)
            table = ghost_crows if ghost else crows
            table = table[pl.ds(pl.multiple_of(at * TERMS, TERMS), TERMS), :]
            left_side = jnp.concatenate(parts_of(table * scales[1, index, 0:TERMS, :], 2), axis=0)
            left_side = left_side.astype(BF16)
            total = total + jnp.dot(
                jnp.concatenate([left_side, left_side], axis=1),
                slopes[256 * m : 256 * (m + 1), :],
                preferred_element_type=F32,
            )
        total = total[0:16] + total[16:32]
        for half in range(2):
            at = pl.ds(pl.multiple_of(n * 16, 16), 16)
            sums[half, at, :] = total[:, 128 * half : 128 * (half + 1)]

    def put_slopes(n, slopes):
        following = jnp.minimum(n + 1, 15)
        for m in range(9):
            for at in range(0, 128, 32):
                y = jnp.maximum(dist[m, at : at + 32, :], 1e-12)
                inverse = lax.rsqrt(y)
                q = y * inverse
                reach = jnp.maximum(2.0 - q, 0.0)
                slope = jnp.where(y < 1.0, 4.0 - 3.0 * q, reach * reach * inverse)
                soft = lax.rsqrt(y + 4.0 * SOFTENING)
                damped = slope * (y * (soft * soft))
                both = jnp.concatenate([slope, damped], axis=1)
                high = both.astype(BF16)
                base = 256 * m + at
                slopes[base : base + 32, :] = high
                slopes[base + 128 : base + 160, :] = (both - high.astype(F32)).astype(BF16)
            force_measure(following, m)

    def force_step(n, carry):
        gather_sums(jnp.maximum(2 * n - 1, 0), odd_slopes)
        put_slopes(2 * n, even_slopes)
        gather_sums(2 * n, even_slopes)
        put_slopes(2 * n + 1, odd_slopes)
        return carry

    for m in range(9):
        force_measure(0, m)
    lax.fori_loop(0, 8, force_step, 0)
    gather_sums(15, odd_slopes)

    for row in range(2):
        mass = fields[row, 6, 0:8, :]
        valid = mass > 0.0
        rho = rhos[row * PLACES : row * PLACES + 8, :]
        density[row] = jnp.where(valid, rho, 0.0)
        inverse_rho = 1.0 / jnp.where(valid, rho, 1.0)

        def term(k, half):
            return sums[half, pl.ds(row * 128 + k, 8, stride=16), :]

        mass_sum, share_sum, drag_sum = term(0, 0), term(6, 0), term(6, 1)
        pressure_scale = -3.0 * KERNEL_NORM * -SOUND_SQ * 0.5
        viscous_scale = -3.0 * KERNEL_NORM * 2.0 * VISCOSITY
        for f in range(3):
            high, low = parts_of(2.0 * fields[row, f, 0:8, :] - 1.0, 2)
            x = high + low
            first = x * mass_sum - term(1 + f, 0)
            second = x * share_sum - term(7 + f, 0)
            if f < 2:
                first = first - 2.0 * term(4 + f, 0)
                second = second - 2.0 * term(10 + f, 0)
            viscous = fields[row, 3 + f, 0:8, :] * drag_sum - term(12 + f, 1)
            value = pressure_scale * (first * inverse_rho + second)
            value = value + viscous_scale * viscous * inverse_rho
            accel[row, f] = jnp.where(valid, value, 0.0)


def scratch_of(tables, rows):
    return [
        pltpu.VMEM((t.shape[0] // 2 * rows, *t.shape[1:]), t.dtype) for t in tables
    ]


def params(mib):
    return pltpu.CompilerParams(vmem_limit_bytes=mib * 2**20)


def local(rows_axis, columns_axis, position, velocity, particle_mass, cell_counts, shear_shift):
    slabs, blocks = lax.axis_size(rows_axis), lax.axis_size(columns_axis)
    axes = (rows_axis, columns_axis)
    half = blocks // 2
    slab = lax.axis_index(rows_axis)
    past = shear_shift[0] - half * particle_mass.shape[1]

    ring = [(i, (i + 1) % blocks) for i in range(blocks)]
    fields = jnp.concatenate(
        [
            jnp.transpose(position, (0, 3, 1, 2)),
            jnp.transpose(velocity, (0, 3, 1, 2)),
            particle_mass[:, None],
        ],
        axis=1,
    )
    field = lax.broadcasted_iota(jnp.int32, fields.shape, 1)
    slot = lax.broadcasted_iota(jnp.int32, fields.shape, 3)
    fields = jnp.where((field < 6) | (slot < cell_counts[:, None, :, None]), fields, 0.0)
    shapes = (*TABLES, jax.ShapeDtypeStruct((2 * PLACES, 128), F32))

    def tables_call(kernel, run, inputs, tables, blocks):
        count = len(inputs) + 1
        return pl.pallas_call(
            kernel,
            out_shape=shapes,
            in_specs=[SMEM] + [VMEM] * (len(inputs) + len(tables)),
            out_specs=[VMEM] * 5,
            scratch_shapes=[
                pltpu.VMEM((2 * PLACES * DEPTH, 128), F32),
                pltpu.VMEM((1, 9, DEPTH, 128), F32),
                pltpu.VMEM((blocks, 128, 128), F32),
            ],
            input_output_aliases={count + n: n for n in range(len(tables))},
            compiler_params=params(8),
            cost_estimate=pl.CostEstimate(
                flops=100_000_000, bytes_accessed=4_000_000, transcendentals=1_000_000
            ),
        )(run.astype(jnp.int32)[None], *inputs, *tables)

    block = lax.axis_index(columns_axis)
    edge = (slab == 0) | (slab == slabs - 1)
    corner = (block == 0) & (slab == 0)
    ahead, late = (block == 0) & ~corner, edge & (block >= half)
    own_now = [ahead, ~(ahead | late | corner), late, corner]
    beside_now = [~corner, corner]

    def own_work(which, tables):
        return tables_call(own_kernel, own_now[which], (fields,), tables, 6)

    def beside_work(which, tables):
        return tables_call(beside_kernel, beside_now[which], (left, right), tables, 8)

    left = lax.ppermute(fields, columns_axis, ring)
    tables = own_work(0, ())
    right = lax.ppermute(fields, columns_axis, [(j, i) for i, j in ring])
    tables = own_work(1, tables)

    odd = lax.rem(slab, 2)
    start = 6 + jnp.where(slab == slabs - 1, past, jnp.where(slab == 0, -past, 0))
    info = jnp.stack([odd, start]).astype(jnp.int32)
    sent = jax.ShapeDtypeStruct((SENT, 128), F32)
    far, same = pl.pallas_call(
        window_kernel,
        out_shape=(sent, sent),
        in_specs=[SMEM, VMEM, VMEM, VMEM],
        out_specs=(VMEM, VMEM),
        compiler_params=params(4),
        name="window",
    )(info, left, fields, right)

    same_pairs, far_pairs = [], []
    for s in range(slabs):
        for b in range(blocks):
            me = s * blocks + b
            same_pairs.append((me, (s + 1 if s % 2 == 0 else s - 1) * blocks + b))
            other, to = (s - 1, b) if s % 2 == 0 else (s + 1, b)
            if other < 0 or other >= slabs:
                other, to = other % slabs, (b + half) % blocks
            far_pairs.append((me, other * blocks + to))
    far = lax.ppermute(far, axes, far_pairs)
    tables = own_work(2, tables)
    tables = beside_work(0, tables)
    same = lax.ppermute(same, axes, same_pairs)
    tables = own_work(3, tables)
    tables = beside_work(1, tables)

    jump = jnp.where(slab == slabs - 1, SHEAR_JUMP, jnp.where(slab == 0, -SHEAR_JUMP, 0.0))
    density, accel = pl.pallas_call(
        late_kernel,
        out_shape=(
            jax.ShapeDtypeStruct((2, 8, 128), F32),
            jax.ShapeDtypeStruct((2, 3, 8, 128), F32),
        ),
        in_specs=[SMEM, SMEM] + [VMEM] * 7,
        out_specs=(VMEM, VMEM),
        scratch_shapes=[
            *scratch_of(TABLES, 4),
            pltpu.VMEM((4 * PLACES * DEPTH, 128), F32),
            pltpu.VMEM((2, 9, DEPTH, 128), F32),
            pltpu.VMEM((2 * PLACES, 128), F32),
            pltpu.VMEM((2 * PLACES, 128), F32),
            pltpu.VMEM((2 * PLACES * TERMS, 128), F32),
            pltpu.VMEM((2 * PLACES * TERMS, 128), F32),
            pltpu.VMEM((12, 128, 128), F32),
            pltpu.VMEM((2, 16 * 16, 128), F32),
            pltpu.VMEM((9 * 256, 256), BF16),
            pltpu.VMEM((9 * 256, 256), BF16),
        ],
        compiler_params=params(24),
        name="late",
    )(info, jump.astype(F32)[None], far, same, *tables)
    return (density, jnp.transpose(accel, (0, 2, 3, 1)))


def solution(mesh):
    placed = (
        P("gy", "gx", None, None),
        P("gy", "gx", None, None),
        P("gy", "gx", None),
        P("gy", "gx"),
        P(),
    )

    def step(*args):
        return local("gy", "gx", *args)

    return jax.shard_map(
        step,
        mesh=mesh,
        in_specs=placed,
        out_specs=(P("gy", "gx", None), P("gy", "gx", None, None)),
        check_vma=False,
    )
```

```python
import functools
import math

import jax
import jax.numpy as jnp
from jax import lax
from jax.experimental import pallas as pl
from jax.experimental.pallas import tpu as pltpu
from jax.sharding import PartitionSpec as P


SMOOTHING = 0.5
KERNEL_NORM = 1.0 / (math.pi * SMOOTHING**3)
SOUND_SQ = 0.2
VISCOSITY = 0.05
SOFTENING = 0.0025
SHEAR_JUMP = 1.0

COLS, PLACES = 12, 16
DEPTH = 32
TERMS = 16
NEAR = 7
SENT = 136
BF16, F32 = jnp.bfloat16, jnp.float32
NEIGHBOURS = [(a, b) for a in (-1, 0, 1) for b in (-1, 0, 1)]
VMEM = pl.BlockSpec(memory_space=pltpu.VMEM)
SMEM = pl.BlockSpec(memory_space=pltpu.SMEM)
TABLES = (
    jax.ShapeDtypeStruct((2, 7, PLACES, 128), F32),
    jax.ShapeDtypeStruct((2 * PLACES * DEPTH, 128), F32),
    jax.ShapeDtypeStruct((2 * COLS, 128, DEPTH), BF16),
    jax.ShapeDtypeStruct((2 * COLS, 128, 128), F32),
)


def place_of(column):
    return column & (PLACES - 1)


def window_kernel(info, left, own, right, far_out, same_out):
    odd, start = info[0], info[1]
    for out in (far_out, same_out):
        near_row = jnp.where(odd == 1, 1, 0)
        if out is same_out:
            near_row = 1 - near_row
        place = 0
        for row, fields in ((near_row, range(NEAR)), (1 - near_row, (0, 1, 2, 6))):
            for f in fields:
                wide = jnp.concatenate([left[row, f], own[row, f], right[row, f]], axis=0)
                if out is same_out:
                    piece = wide[6:18]
                else:
                    piece = pltpu.roll(wide, 24 - start, 0)[0:COLS]
                out[place : place + COLS, :] = piece
                place += COLS
        out[place:SENT, :] = jnp.zeros((SENT - place, 128), F32)


def parts_of(x, count):
    parts = []
    for _ in range(count - 1):
        part = x.astype(BF16).astype(F32)
        parts.append(part)
        x = x - part
    parts.append(x.astype(BF16).astype(F32))
    return parts


def fill_scales(scales):
    k = lax.broadcasted_iota(jnp.int32, (DEPTH, 128), 0)
    for n, (a, b) in enumerate(NEIGHBOURS):
        scale = jnp.where(k < 18, 1.0, 0.0)
        scale = jnp.where((k >= 18) & (k < 22), float(b), scale)
        scale = jnp.where((k >= 22) & (k < 26), float(a), scale)
        scale = jnp.where(k == 26, float(a * a + b * b), scale)
        scales[0, n] = scale
        if scales.shape[0] > 1:
            scale = jnp.where((k == 4) | (k == 10) | (k == 20) | (k == 26), float(b), 1.0)
            scale = jnp.where((k == 5) | (k == 11) | (k == 21) | (k == 27), float(a), scale)
            scales[1, n] = scale


def build_tables(rows, halves, fields, irows, jcols, masses, jrows, irows_of=None):
    irows_of = rows if irows_of is None else irows_of
    k = lax.broadcasted_iota(jnp.int32, (DEPTH, 128), 0)
    ones_j = jnp.where(((k >= 15) & (k < 20)) | (k == 22) | (k == 23) | (k == 26), 1.0, 0.0)
    ones_i = jnp.where((k >= 12) & (k < 15), 1.0, 0.0)
    ones_i = jnp.where((k == 20) | (k == 21) | (k >= 24) & (k < 27), 4.0, ones_i)
    pick_mass = jnp.where((k >= 27) & (k < 30), 1.0, 0.0).astype(BF16)

    count = len(halves)

    def build(n, carry, with_irows=True):
        row, half = n // count, n % count + halves[0]
        step = row * 2 + half
        base = pl.multiple_of(step * (8 * DEPTH), 8 * DEPTH)
        cells = pl.ds(pl.multiple_of(half * 8, 8), 8)
        for c in range(8):
            jrows[pl.ds(base + c * DEPTH, DEPTH), :] = ones_j
            if with_irows:
                irows[pl.ds(base + c * DEPTH, DEPTH), :] = ones_i

        def put(table, k, value):
            if table is irows and not with_irows:
                return
            table[pl.ds(base + k, 8, stride=DEPTH), :] = value

        norm = jnp.zeros((8, 128), F32)
        for f in range(3):
            x = 2.0 * fields[row, f, cells, :] - 1.0
            high, low = parts_of(x, 2)
            both = high + low
            norm = norm + both * both
            for k, (mine, other) in enumerate(((high, high), (high, low), (low, high), (low, low))):
                put(jrows, 4 * f + k, mine)
                put(irows, 4 * f + k, -2.0 * other)
            if f < 2:
                at = 18 + 4 * f
                put(jrows, at + 2, high)
                put(jrows, at + 3, low)
                put(irows, at, -4.0 * high)
                put(irows, at + 1, -4.0 * low)
        for k, part in enumerate(parts_of(norm, 3)):
            put(jrows, 12 + k, part)
            put(irows, 15 + k, part)
        for k, part in enumerate(parts_of(fields[row, 6, cells, :], 3)):
            put(jrows, 27 + k, part)
        return carry

    lax.fori_loop(0, irows_of * count, build, 0)
    if irows_of < rows:
        rest = functools.partial(build, with_irows=False)
        lax.fori_loop(irows_of * count, rows * count, rest, 0)

    def turn_rows(pair, carry):
        for n in range(48):
            row, column = 2 * pair + n % 2, n // 2 - 2
            if column > 9 or (0 if 0 <= column < 8 else 1) not in halves:
                continue
            c = column + 2
            cell = row * PLACES + place_of(column)
            table = jrows[pl.ds(pl.multiple_of(cell * DEPTH, DEPTH), DEPTH), :]
            flipped = table.T.astype(BF16)
            jcols[row * COLS + c] = flipped
            masses[row * COLS + c] = jnp.dot(flipped, pick_mass, preferred_element_type=F32)
        return carry

    lax.fori_loop(0, rows // 2, turn_rows, 0)


def rows_of(table, cell):
    return table[pl.ds(pl.multiple_of(cell * DEPTH, DEPTH), DEPTH), :]


def put_distances(dist, m, table, scale, columns):
    right_side = (table * scale).astype(BF16)
    dist[m] = jnp.dot(columns, right_side, preferred_element_type=F32)


def add_density(total, dist, m, masses, cell):
    for at in range(0, 128, 32):
        y = jnp.maximum(dist[m, at : at + 32, :], 1e-12)
        q = y * lax.rsqrt(y)
        reach = jnp.maximum(2.0 - q, 0.0)
        inner = 4.0 - 3.0 * y * reach
        outer = reach * reach * reach
        w = jnp.where(y < 1.0, inner, outer) * masses[cell, at : at + 32, :]
        total = total + ((w[0:8] + w[8:16]) + (w[16:24] + w[24:32]))
    return total


def density_of(total):
    return jnp.sum(total, axis=0, keepdims=True) * (0.25 * KERNEL_NORM)


def row_index(direction, b):
    return direction * 3 + b + 1


def own_kernel(run, own, *refs):
    fields, irows, jcols, masses, rhos, jrows, scales, dist = refs[-8:]

    @pl.when(run[0] == 1)
    def _():
        fields[...] = jnp.zeros_like(fields)
        for row in range(2):
            for f in range(7):
                fields[row, f, 0:8, :] = own[row, f]
        fill_scales(scales)
        build_tables(2, (0,), fields, irows, jcols, masses, jrows)
        for at in (1, 10, COLS + 1, COLS + 10):
            jcols[at] = jnp.zeros((128, DEPTH), BF16)
            masses[at] = jnp.zeros((128, 128), F32)

        def blocks(n):
            side, column = n // 8, n % 8
            found = [
                (row_index(direction, b), row * COLS + column + (b + 2))
                for direction, row in ((1, side), (2 - 2 * side, 1 - side))
                for b in (-1, 0, 1)
            ]
            return side * PLACES + column, found

        def measure(n, m):
            cell, near = blocks(n)
            columns = jcols[near[m][1]]
            put_distances(dist, m, rows_of(irows, cell), scales[0, near[m][0]], columns)

        def step(n, carry):
            cell, near = blocks(n)
            following = jnp.minimum(n + 1, 15)
            total = jnp.zeros((8, 128), F32)
            for m in range(6):
                total = add_density(total, dist, m, masses, near[m][1])
                measure(following, m)
            rhos[pl.ds(cell, 1), :] = density_of(total)
            return carry

        rhos[...] = jnp.zeros_like(rhos)
        for m in range(6):
            measure(0, m)
        lax.fori_loop(0, 16, step, 0, unroll=2)


def beside_kernel(run, left, right, *refs):
    fields, irows, jcols, masses, rhos, jrows, scales, dist = refs[-8:]

    @pl.when(run[0] == 1)
    def _():
        for row in range(2):
            for f in range(7):
                fields[row, f, 8:10, :] = right[row, f, 0:2, :]
                fields[row, f, 14:16, :] = left[row, f, 6:8, :]
        fill_scales(scales)
        build_tables(2, (1,), fields, irows, jcols, masses, jrows)

        def blocks(n):
            side, far = n // 2, n % 2
            outer, inner = jnp.where(far == 1, 8, -1), jnp.where(far == 1, 7, 0)
            found = []
            for direction, row in ((1, side), (2 - 2 * side, 1 - side)):
                for b in (-1, 0, 1):
                    found.append((0, row_index(direction, b), row * COLS + outer + (b + 2)))
                at = row * COLS + outer + 2
                found.append((1, row_index(direction, 2 * far - 1), at))
            cells = [side * PLACES + place_of(column) for column in (outer, inner)]
            return cells, found

        def measure(n, m):
            cells, near = blocks(n)
            which, index, at = near[m]
            table = rows_of(irows, cells[which])
            put_distances(dist, m, table, scales[0, index], jcols[at])

        def step(n, carry):
            cells, near = blocks(n)
            following = jnp.minimum(n + 1, 3)
            totals = [jnp.zeros((8, 128), F32)] * 2
            for m in range(8):
                which, _, at = near[m]
                totals[which] = add_density(totals[which], dist, m, masses, at)
                measure(following, m)
            rhos[pl.ds(cells[0], 1), :] = density_of(totals[0])
            rhos[pl.ds(cells[1], 1), :] = density_of(totals[1]) + rhos[pl.ds(cells[1], 1), :]
            return carry

        for m in range(8):
            measure(0, m)
        lax.fori_loop(0, 4, step, 0)


def late_kernel(
    info, jump_ref, far, same, fields, irows, jcols, masses, partial, density, accel,
    ghosts, ghost_irows, ghost_jcols, ghost_masses, jrows,
    scales, rhos, ghost_rhos, crows, ghost_crows, dist, sums, even_slopes, odd_slopes,
):
    odd, jump = info[0], jump_ref[0]

    ghosts[...] = jnp.zeros_like(ghosts)
    for piece, side in ((same, 1 - odd), (far, odd)):
        for f in range(NEAR):
            value = piece[f * COLS : (f + 1) * COLS, :]
            if piece is far and f == 3:
                value = value + jump
            ghosts[side, f, 0:8, :] = value[2:10]
            ghosts[side, f, 8:10, :] = value[10:12]
            ghosts[side, f, 14:16, :] = value[0:2]
        for n, f in enumerate((0, 1, 2, 6)):
            at = (NEAR + n) * COLS
            value = piece[at : at + COLS, :]
            ghosts[2 + side, f, 0:8, :] = value[2:10]
            ghosts[2 + side, f, 8:10, :] = value[10:12]
            ghosts[2 + side, f, 14:16, :] = value[0:2]
    fill_scales(scales)
    build_tables(4, (0, 1), ghosts, ghost_irows, ghost_jcols, ghost_masses, jrows, 2)

    def blocks(n):
        side, column = n // 10, n % 10 - 1
        return side * PLACES + place_of(column), side, [
            (who, row_index(direction, b), row * COLS + column + (b + 2))
            for who, direction, row in (
                ("far", 2 * side, side + 2),
                ("near", 1, side),
                ("own", 2 - 2 * side, side),
                ("mine", 2 * side, side),
            )
            for b in (-1, 0, 1)
        ]

    def measure(n, m):
        cell, _, near = blocks(n)
        who, index, at = near[m]
        table = rows_of(irows if who == "mine" else ghost_irows, cell)
        columns = (jcols if who == "own" else ghost_jcols)[at]
        put_distances(dist, m, table, scales[0, index], columns)

    def density_step(n, carry):
        cell, _, near = blocks(n)
        following = jnp.minimum(n + 1, 19)
        ghost_total = jnp.zeros((8, 128), F32)
        own_total = jnp.zeros((8, 128), F32)
        for m in range(12):
            who, _, at = near[m]
            which = masses if who == "own" else ghost_masses
            if who == "mine":
                own_total = add_density(own_total, dist, m, which, at)
            else:
                ghost_total = add_density(ghost_total, dist, m, which, at)
            measure(following, m)
        ghost_rhos[pl.ds(cell, 1), :] = density_of(ghost_total)
        rhos[pl.ds(cell, 1), :] = density_of(own_total) + partial[pl.ds(cell, 1), :]
        return carry

    rhos[...] = jnp.zeros_like(rhos)
    ghost_rhos[...] = jnp.zeros_like(ghost_rhos)
    for m in range(12):
        measure(0, m)
    lax.fori_loop(0, 20, density_step, 0, unroll=2)

    def coefficients(source, densities, target):
        def step(n, carry):
            row, half = n // 2, n % 2
            base = n * (8 * TERMS)
            cells = pl.ds(pl.multiple_of(half * 8, 8), 8)
            mass = source[row, 6, cells, :]
            rho = densities[pl.ds(pl.multiple_of(n * 8, 8), 8), :]
            share = mass / jnp.where(mass > 0.0, rho, 1.0)
            terms = []
            for weight in (mass, share):
                terms.append(weight)
                for f in range(3):
                    high, low = parts_of(2.0 * source[row, f, cells, :] - 1.0, 2)
                    terms.append(weight * (high + low))
                terms.append(weight)
                terms.append(weight)
            for f in range(3, 6):
                terms.append(share * source[row, f, cells, :])
            terms.append(jnp.zeros((8, 128), F32))
            for t, term in enumerate(terms):
                target[pl.ds(base + t, 8, stride=TERMS), :] = term
            return carry

        lax.fori_loop(0, 4, step, 0)

    coefficients(fields, rhos, crows)
    coefficients(ghosts, ghost_rhos, ghost_crows)

    def force_blocks(n):
        side, column = n // 8, n % 8
        return side * PLACES + column, [
            (ghost, row_index(direction, b), row, column + b)
            for ghost, direction, row in (
                (True, 2 * side, side),
                (False, 1, side),
                (False, 2 - 2 * side, 1 - side),
            )
            for b in (-1, 0, 1)
        ]

    def force_measure(n, m):
        cell, near = force_blocks(n)
        ghost, index, row, column = near[m]
        columns = (ghost_jcols if ghost else jcols)[row * COLS + column + 2]
        put_distances(dist, m, rows_of(irows, cell), scales[0, index], columns)

    def gather_sums(n, slopes):
        _, near = force_blocks(n)
        total = jnp.zeros((DEPTH, 256), F32)
        for m in range(9):
            ghost, index, row, column = near[m]
            at = row * PLACES + place_of(column)
            table = ghost_crows if ghost else crows
            table = table[pl.ds(pl.multiple_of(at * TERMS, TERMS), TERMS), :]
            left_side = jnp.concatenate(parts_of(table * scales[1, index, 0:TERMS, :], 2), axis=0)
            left_side = left_side.astype(BF16)
            total = total + jnp.dot(
                jnp.concatenate([left_side, left_side], axis=1),
                slopes[256 * m : 256 * (m + 1), :],
                preferred_element_type=F32,
            )
        total = total[0:16] + total[16:32]
        for half in range(2):
            at = pl.ds(pl.multiple_of(n * 16, 16), 16)
            sums[half, at, :] = total[:, 128 * half : 128 * (half + 1)]

    def put_slopes(n, slopes):
        following = jnp.minimum(n + 1, 15)
        for m in range(9):
            for at in range(0, 128, 32):
                y = jnp.maximum(dist[m, at : at + 32, :], 1e-12)
                inverse = lax.rsqrt(y)
                q = y * inverse
                reach = jnp.maximum(2.0 - q, 0.0)
                slope = jnp.where(y < 1.0, 4.0 - 3.0 * q, reach * reach * inverse)
                soft = lax.rsqrt(y + 4.0 * SOFTENING)
                damped = slope * (y * (soft * soft))
                both = jnp.concatenate([slope, damped], axis=1)
                high = both.astype(BF16)
                base = 256 * m + at
                slopes[base : base + 32, :] = high
                slopes[base + 128 : base + 160, :] = (both - high.astype(F32)).astype(BF16)
            force_measure(following, m)

    def force_step(n, carry):
        gather_sums(jnp.maximum(2 * n - 1, 0), odd_slopes)
        put_slopes(2 * n, even_slopes)
        gather_sums(2 * n, even_slopes)
        put_slopes(2 * n + 1, odd_slopes)
        return carry

    for m in range(9):
        force_measure(0, m)
    lax.fori_loop(0, 8, force_step, 0)
    gather_sums(15, odd_slopes)

    for row in range(2):
        mass = fields[row, 6, 0:8, :]
        valid = mass > 0.0
        rho = rhos[row * PLACES : row * PLACES + 8, :]
        density[row] = jnp.where(valid, rho, 0.0)
        inverse_rho = 1.0 / jnp.where(valid, rho, 1.0)

        def term(k, half):
            return sums[half, pl.ds(row * 128 + k, 8, stride=16), :]

        mass_sum, share_sum, drag_sum = term(0, 0), term(6, 0), term(6, 1)
        pressure_scale = -3.0 * KERNEL_NORM * -SOUND_SQ * 0.5
        viscous_scale = -3.0 * KERNEL_NORM * 2.0 * VISCOSITY
        for f in range(3):
            high, low = parts_of(2.0 * fields[row, f, 0:8, :] - 1.0, 2)
            x = high + low
            first = x * mass_sum - term(1 + f, 0)
            second = x * share_sum - term(7 + f, 0)
            if f < 2:
                first = first - 2.0 * term(4 + f, 0)
                second = second - 2.0 * term(10 + f, 0)
            viscous = fields[row, 3 + f, 0:8, :] * drag_sum - term(12 + f, 1)
            value = pressure_scale * (first * inverse_rho + second)
            value = value + viscous_scale * viscous * inverse_rho
            accel[row, f] = jnp.where(valid, value, 0.0)


def scratch_of(tables, rows):
    return [
        pltpu.VMEM((t.shape[0] // 2 * rows, *t.shape[1:]), t.dtype) for t in tables
    ]


def params(mib):
    return pltpu.CompilerParams(vmem_limit_bytes=mib * 2**20)


def local(rows_axis, columns_axis, position, velocity, particle_mass, cell_counts, shear_shift):
    slabs, blocks = lax.axis_size(rows_axis), lax.axis_size(columns_axis)
    axes = (rows_axis, columns_axis)
    half = blocks // 2
    slab = lax.axis_index(rows_axis)
    past = shear_shift[0] - half * particle_mass.shape[1]

    ring = [(i, (i + 1) % blocks) for i in range(blocks)]
    fields = jnp.concatenate(
        [
            jnp.transpose(position, (0, 3, 1, 2)),
            jnp.transpose(velocity, (0, 3, 1, 2)),
            particle_mass[:, None],
        ],
        axis=1,
    )
    field = lax.broadcasted_iota(jnp.int32, fields.shape, 1)
    slot = lax.broadcasted_iota(jnp.int32, fields.shape, 3)
    fields = jnp.where((field < 6) | (slot < cell_counts[:, None, :, None]), fields, 0.0)
    shapes = (*TABLES, jax.ShapeDtypeStruct((2 * PLACES, 128), F32))

    def tables_call(kernel, run, inputs, tables, blocks):
        count = len(inputs) + 1
        return pl.pallas_call(
            kernel,
            out_shape=shapes,
            in_specs=[SMEM] + [VMEM] * (len(inputs) + len(tables)),
            out_specs=[VMEM] * 5,
            scratch_shapes=[
                pltpu.VMEM((2 * PLACES * DEPTH, 128), F32),
                pltpu.VMEM((1, 9, DEPTH, 128), F32),
                pltpu.VMEM((blocks, 128, 128), F32),
            ],
            input_output_aliases={count + n: n for n in range(len(tables))},
            compiler_params=params(8),
            cost_estimate=pl.CostEstimate(
                flops=100_000_000, bytes_accessed=4_000_000, transcendentals=1_000_000
            ),
        )(run.astype(jnp.int32)[None], *inputs, *tables)

    block = lax.axis_index(columns_axis)
    edge = (slab == 0) | (slab == slabs - 1)
    corner = (block == 0) & (slab == 0)
    ahead, late = (block == 0) & ~corner, edge & (block >= half)
    own_now = [ahead, ~(ahead | late | corner), late, corner]
    beside_now = [~corner, corner]

    def own_work(which, tables):
        return tables_call(own_kernel, own_now[which], (fields,), tables, 6)

    def beside_work(which, tables):
        return tables_call(beside_kernel, beside_now[which], (left, right), tables, 8)

    left = lax.ppermute(fields, columns_axis, ring)
    tables = own_work(0, ())
    right = lax.ppermute(fields, columns_axis, [(j, i) for i, j in ring])
    tables = own_work(1, tables)

    odd = lax.rem(slab, 2)
    start = 6 + jnp.where(slab == slabs - 1, past, jnp.where(slab == 0, -past, 0))
    info = jnp.stack([odd, start]).astype(jnp.int32)
    sent = jax.ShapeDtypeStruct((SENT, 128), F32)
    far, same = pl.pallas_call(
        window_kernel,
        out_shape=(sent, sent),
        in_specs=[SMEM, VMEM, VMEM, VMEM],
        out_specs=(VMEM, VMEM),
        compiler_params=params(4),
        name="window",
    )(info, left, fields, right)

    same_pairs, far_pairs = [], []
    for s in range(slabs):
        for b in range(blocks):
            me = s * blocks + b
            same_pairs.append((me, (s + 1 if s % 2 == 0 else s - 1) * blocks + b))
            other, to = (s - 1, b) if s % 2 == 0 else (s + 1, b)
            if other < 0 or other >= slabs:
                other, to = other % slabs, (b + half) % blocks
            far_pairs.append((me, other * blocks + to))
    far = lax.ppermute(far, axes, far_pairs)
    tables = own_work(2, tables)
    tables = beside_work(0, tables)
    same = lax.ppermute(same, axes, same_pairs)
    tables = own_work(3, tables)
    tables = beside_work(1, tables)

    jump = jnp.where(slab == slabs - 1, SHEAR_JUMP, jnp.where(slab == 0, -SHEAR_JUMP, 0.0))
    density, accel = pl.pallas_call(
        late_kernel,
        out_shape=(
            jax.ShapeDtypeStruct((2, 8, 128), F32),
            jax.ShapeDtypeStruct((2, 3, 8, 128), F32),
        ),
        in_specs=[SMEM, SMEM] + [VMEM] * 7,
        out_specs=(VMEM, VMEM),
        scratch_shapes=[
            *scratch_of(TABLES[:1], 4),
            *scratch_of(TABLES[1:2], 2),
            *scratch_of(TABLES[2:], 4),
            pltpu.VMEM((4 * PLACES * DEPTH, 128), F32),
            pltpu.VMEM((2, 9, DEPTH, 128), F32),
            pltpu.VMEM((2 * PLACES, 128), F32),
            pltpu.VMEM((2 * PLACES, 128), F32),
            pltpu.VMEM((2 * PLACES * TERMS, 128), F32),
            pltpu.VMEM((2 * PLACES * TERMS, 128), F32),
            pltpu.VMEM((12, 128, 128), F32),
            pltpu.VMEM((2, 16 * 16, 128), F32),
            pltpu.VMEM((9 * 256, 256), BF16),
            pltpu.VMEM((9 * 256, 256), BF16),
        ],
        compiler_params=params(24),
        name="late",
    )(info, jump.astype(F32)[None], far, same, *tables)
    return (density, jnp.transpose(accel, (0, 2, 3, 1)))


def solution(mesh):
    placed = (
        P("gy", "gx", None, None),
        P("gy", "gx", None, None),
        P("gy", "gx", None),
        P("gy", "gx"),
        P(),
    )

    def step(*args):
        return local("gy", "gx", *args)

    return jax.shard_map(
        step,
        mesh=mesh,
        in_specs=placed,
        out_specs=(P("gy", "gx", None), P("gy", "gx", None, None)),
        check_vma=False,
    )
```

```python
import functools
import math

import jax
import jax.numpy as jnp
from jax import lax
from jax.experimental import pallas as pl
from jax.experimental.pallas import tpu as pltpu
from jax.sharding import PartitionSpec as P


SMOOTHING = 0.5
KERNEL_NORM = 1.0 / (math.pi * SMOOTHING**3)
SOUND_SQ = 0.2
VISCOSITY = 0.05
SOFTENING = 0.0025
SHEAR_JUMP = 1.0

COLS, PLACES = 12, 16
DEPTH = 32
TERMS = 16
NEAR = 7
SENT = 136
BF16, F32 = jnp.bfloat16, jnp.float32
NEIGHBOURS = [(a, b) for a in (-1, 0, 1) for b in (-1, 0, 1)]
VMEM = pl.BlockSpec(memory_space=pltpu.VMEM)
SMEM = pl.BlockSpec(memory_space=pltpu.SMEM)
TABLES = (
    jax.ShapeDtypeStruct((2, 7, PLACES, 128), F32),
    jax.ShapeDtypeStruct((2 * PLACES * DEPTH, 128), F32),
    jax.ShapeDtypeStruct((2 * COLS, 128, DEPTH), BF16),
    jax.ShapeDtypeStruct((2 * COLS, 128, 128), F32),
)


def place_of(column):
    return column & (PLACES - 1)


def window_kernel(info, left, own, right, far_out, same_out):
    odd, start = info[0], info[1]
    for out in (far_out, same_out):
        near_row = jnp.where(odd == 1, 1, 0)
        if out is same_out:
            near_row = 1 - near_row
        place = 0
        for row, fields in ((near_row, range(NEAR)), (1 - near_row, (0, 1, 2, 6))):
            for f in fields:
                wide = jnp.concatenate([left[row, f], own[row, f], right[row, f]], axis=0)
                if out is same_out:
                    piece = wide[6:18]
                else:
                    piece = pltpu.roll(wide, 24 - start, 0)[0:COLS]
                out[place : place + COLS, :] = piece
                place += COLS
        out[place:SENT, :] = jnp.zeros((SENT - place, 128), F32)


def parts_of(x, count):
    parts = []
    for _ in range(count - 1):
        part = x.astype(BF16).astype(F32)
        parts.append(part)
        x = x - part
    parts.append(x.astype(BF16).astype(F32))
    return parts


def fill_scales(scales):
    k = lax.broadcasted_iota(jnp.int32, (DEPTH, 128), 0)
    for n, (a, b) in enumerate(NEIGHBOURS):
        scale = jnp.where(k < 18, 1.0, 0.0)
        scale = jnp.where((k >= 18) & (k < 22), float(b), scale)
        scale = jnp.where((k >= 22) & (k < 26), float(a), scale)
        scale = jnp.where(k == 26, float(a * a + b * b), scale)
        scales[0, n] = scale
        if scales.shape[0] > 1:
            scale = jnp.where((k == 4) | (k == 10) | (k == 20) | (k == 26), float(b), 1.0)
            scale = jnp.where((k == 5) | (k == 11) | (k == 21) | (k == 27), float(a), scale)
            scales[1, n] = scale


def build_tables(rows, halves, fields, irows, jcols, masses, jrows, irows_of=None):
    irows_of = rows if irows_of is None else irows_of
    k = lax.broadcasted_iota(jnp.int32, (DEPTH, 128), 0)
    ones_j = jnp.where(((k >= 15) & (k < 20)) | (k == 22) | (k == 23) | (k == 26), 1.0, 0.0)
    ones_i = jnp.where((k >= 12) & (k < 15), 1.0, 0.0)
    ones_i = jnp.where((k == 20) | (k == 21) | (k >= 24) & (k < 27), 4.0, ones_i)
    pick_mass = jnp.where((k >= 27) & (k < 30), 1.0, 0.0).astype(BF16)

    count = len(halves)

    def build(n, carry, with_irows=True):
        row, half = n // count, n % count + halves[0]
        step = row * 2 + half
        base = pl.multiple_of(step * (8 * DEPTH), 8 * DEPTH)
        cells = pl.ds(pl.multiple_of(half * 8, 8), 8)
        for c in range(8):
            jrows[pl.ds(base + c * DEPTH, DEPTH), :] = ones_j
            if with_irows:
                irows[pl.ds(base + c * DEPTH, DEPTH), :] = ones_i

        def put(table, k, value):
            if table is irows and not with_irows:
                return
            table[pl.ds(base + k, 8, stride=DEPTH), :] = value

        norm = jnp.zeros((8, 128), F32)
        for f in range(3):
            x = 2.0 * fields[row, f, cells, :] - 1.0
            high, low = parts_of(x, 2)
            both = high + low
            norm = norm + both * both
            for k, (mine, other) in enumerate(((high, high), (high, low), (low, high), (low, low))):
                put(jrows, 4 * f + k, mine)
                put(irows, 4 * f + k, -2.0 * other)
            if f < 2:
                at = 18 + 4 * f
                put(jrows, at + 2, high)
                put(jrows, at + 3, low)
                put(irows, at, -4.0 * high)
                put(irows, at + 1, -4.0 * low)
        for k, part in enumerate(parts_of(norm, 3)):
            put(jrows, 12 + k, part)
            put(irows, 15 + k, part)
        for k, part in enumerate(parts_of(fields[row, 6, cells, :], 3)):
            put(jrows, 27 + k, part)
        return carry

    lax.fori_loop(0, irows_of * count, build, 0)
    if irows_of < rows:
        rest = functools.partial(build, with_irows=False)
        lax.fori_loop(irows_of * count, rows * count, rest, 0)

    def turn_rows(pair, carry):
        for n in range(48):
            row, column = 2 * pair + n % 2, n // 2 - 2
            if column > 9 or (0 if 0 <= column < 8 else 1) not in halves:
                continue
            c = column + 2
            cell = row * PLACES + place_of(column)
            table = jrows[pl.ds(pl.multiple_of(cell * DEPTH, DEPTH), DEPTH), :]
            flipped = table.T.astype(BF16)
            jcols[row * COLS + c] = flipped
            masses[row * COLS + c] = jnp.dot(flipped, pick_mass, preferred_element_type=F32)
        return carry

    lax.fori_loop(0, rows // 2, turn_rows, 0)


def rows_of(table, cell):
    return table[pl.ds(pl.multiple_of(cell * DEPTH, DEPTH), DEPTH), :]


def put_distances(dist, m, table, scale, columns):
    right_side = (table * scale).astype(BF16)
    dist[m] = jnp.dot(columns, right_side, preferred_element_type=F32)


def add_density(total, dist, m, masses, cell):
    for at in range(0, 128, 32):
        y = jnp.maximum(dist[m, at : at + 32, :], 1e-12)
        q = y * lax.rsqrt(y)
        reach = jnp.maximum(2.0 - q, 0.0)
        inner = 4.0 - 3.0 * y * reach
        outer = reach * reach * reach
        w = jnp.where(y < 1.0, inner, outer) * masses[cell, at : at + 32, :]
        total = total + ((w[0:8] + w[8:16]) + (w[16:24] + w[24:32]))
    return total


def density_of(total):
    return jnp.sum(total, axis=0, keepdims=True) * (0.25 * KERNEL_NORM)


def row_index(direction, b):
    return direction * 3 + b + 1


def own_kernel(run, own, *refs):
    fields, irows, jcols, masses, rhos, jrows, scales, dist = refs[-8:]

    @pl.when(run[0] == 1)
    def _():
        fields[...] = jnp.zeros_like(fields)
        for row in range(2):
            for f in range(7):
                fields[row, f, 0:8, :] = own[row, f]
        fill_scales(scales)
        build_tables(2, (0,), fields, irows, jcols, masses, jrows)
        for at in (1, 10, COLS + 1, COLS + 10):
            jcols[at] = jnp.zeros((128, DEPTH), BF16)
            masses[at] = jnp.zeros((128, 128), F32)

        def blocks(n):
            side, column = n // 8, n % 8
            found = [
                (row_index(direction, b), row * COLS + column + (b + 2))
                for direction, row in ((1, side), (2 - 2 * side, 1 - side))
                for b in (-1, 0, 1)
            ]
            return side * PLACES + column, found

        def measure(n, m):
            cell, near = blocks(n)
            columns = jcols[near[m][1]]
            put_distances(dist, m, rows_of(irows, cell), scales[0, near[m][0]], columns)

        def step(n, carry):
            cell, near = blocks(n)
            following = jnp.minimum(n + 1, 15)
            total = jnp.zeros((8, 128), F32)
            for m in range(6):
                total = add_density(total, dist, m, masses, near[m][1])
                measure(following, m)
            rhos[pl.ds(cell, 1), :] = density_of(total)
            return carry

        rhos[...] = jnp.zeros_like(rhos)
        for m in range(6):
            measure(0, m)
        lax.fori_loop(0, 16, step, 0, unroll=2)


def beside_kernel(run, left, right, *refs):
    fields, irows, jcols, masses, rhos, jrows, scales, dist = refs[-8:]

    @pl.when(run[0] == 1)
    def _():
        for row in range(2):
            for f in range(7):
                fields[row, f, 8:10, :] = right[row, f, 0:2, :]
                fields[row, f, 14:16, :] = left[row, f, 6:8, :]
        fill_scales(scales)
        build_tables(2, (1,), fields, irows, jcols, masses, jrows)

        def blocks(n):
            side, far = n // 2, n % 2
            outer, inner = jnp.where(far == 1, 8, -1), jnp.where(far == 1, 7, 0)
            found = []
            for direction, row in ((1, side), (2 - 2 * side, 1 - side)):
                for b in (-1, 0, 1):
                    found.append((0, row_index(direction, b), row * COLS + outer + (b + 2)))
                at = row * COLS + outer + 2
                found.append((1, row_index(direction, 2 * far - 1), at))
            cells = [side * PLACES + place_of(column) for column in (outer, inner)]
            return cells, found

        def measure(n, m):
            cells, near = blocks(n)
            which, index, at = near[m]
            table = rows_of(irows, cells[which])
            put_distances(dist, m, table, scales[0, index], jcols[at])

        def step(n, carry):
            cells, near = blocks(n)
            following = jnp.minimum(n + 1, 3)
            totals = [jnp.zeros((8, 128), F32)] * 2
            for m in range(8):
                which, _, at = near[m]
                totals[which] = add_density(totals[which], dist, m, masses, at)
                measure(following, m)
            rhos[pl.ds(cells[0], 1), :] = density_of(totals[0])
            rhos[pl.ds(cells[1], 1), :] = density_of(totals[1]) + rhos[pl.ds(cells[1], 1), :]
            return carry

        for m in range(8):
            measure(0, m)
        lax.fori_loop(0, 4, step, 0, unroll=2)


def late_kernel(
    info, jump_ref, far, same, fields, irows, jcols, masses, partial, density, accel,
    ghosts, ghost_irows, ghost_jcols, ghost_masses, jrows,
    scales, rhos, ghost_rhos, crows, ghost_crows, dist, sums, even_slopes, odd_slopes,
):
    odd, jump = info[0], jump_ref[0]

    ghosts[...] = jnp.zeros_like(ghosts)
    for piece, side in ((same, 1 - odd), (far, odd)):
        for f in range(NEAR):
            value = piece[f * COLS : (f + 1) * COLS, :]
            if piece is far and f == 3:
                value = value + jump
            ghosts[side, f, 0:8, :] = value[2:10]
            ghosts[side, f, 8:10, :] = value[10:12]
            ghosts[side, f, 14:16, :] = value[0:2]
        for n, f in enumerate((0, 1, 2, 6)):
            at = (NEAR + n) * COLS
            value = piece[at : at + COLS, :]
            ghosts[2 + side, f, 0:8, :] = value[2:10]
            ghosts[2 + side, f, 8:10, :] = value[10:12]
            ghosts[2 + side, f, 14:16, :] = value[0:2]
    fill_scales(scales)
    build_tables(4, (0, 1), ghosts, ghost_irows, ghost_jcols, ghost_masses, jrows, 2)

    def blocks(n):
        side, column = n // 10, n % 10 - 1
        return side * PLACES + place_of(column), side, [
            (who, row_index(direction, b), row * COLS + column + (b + 2))
            for who, direction, row in (
                ("far", 2 * side, side + 2),
                ("near", 1, side),
                ("own", 2 - 2 * side, side),
                ("mine", 2 * side, side),
            )
            for b in (-1, 0, 1)
        ]

    def measure(n, m):
        cell, _, near = blocks(n)
        who, index, at = near[m]
        table = rows_of(irows if who == "mine" else ghost_irows, cell)
        columns = (jcols if who == "own" else ghost_jcols)[at]
        put_distances(dist, m, table, scales[0, index], columns)

    def density_step(n, carry):
        cell, _, near = blocks(n)
        following = jnp.minimum(n + 1, 19)
        ghost_total = jnp.zeros((8, 128), F32)
        own_total = jnp.zeros((8, 128), F32)
        for m in range(12):
            who, _, at = near[m]
            which = masses if who == "own" else ghost_masses
            if who == "mine":
                own_total = add_density(own_total, dist, m, which, at)
            else:
                ghost_total = add_density(ghost_total, dist, m, which, at)
            measure(following, m)
        ghost_rhos[pl.ds(cell, 1), :] = density_of(ghost_total)
        rhos[pl.ds(cell, 1), :] = density_of(own_total) + partial[pl.ds(cell, 1), :]
        return carry

    rhos[...] = jnp.zeros_like(rhos)
    ghost_rhos[...] = jnp.zeros_like(ghost_rhos)
    for m in range(12):
        measure(0, m)
    lax.fori_loop(0, 20, density_step, 0, unroll=4)

    def coefficients(source, densities, target):
        def step(n, carry):
            row, half = n // 2, n % 2
            base = n * (8 * TERMS)
            cells = pl.ds(pl.multiple_of(half * 8, 8), 8)
            mass = source[row, 6, cells, :]
            rho = densities[pl.ds(pl.multiple_of(n * 8, 8), 8), :]
            share = mass / jnp.where(mass > 0.0, rho, 1.0)
            terms = []
            for weight in (mass, share):
                terms.append(weight)
                for f in range(3):
                    high, low = parts_of(2.0 * source[row, f, cells, :] - 1.0, 2)
                    terms.append(weight * (high + low))
                terms.append(weight)
                terms.append(weight)
            for f in range(3, 6):
                terms.append(share * source[row, f, cells, :])
            terms.append(jnp.zeros((8, 128), F32))
            for t, term in enumerate(terms):
                target[pl.ds(base + t, 8, stride=TERMS), :] = term
            return carry

        lax.fori_loop(0, 4, step, 0, unroll=2)

    coefficients(fields, rhos, crows)
    coefficients(ghosts, ghost_rhos, ghost_crows)

    def force_blocks(n):
        side, column = n // 8, n % 8
        return side * PLACES + column, [
            (ghost, row_index(direction, b), row, column + b)
            for ghost, direction, row in (
                (True, 2 * side, side),
                (False, 1, side),
                (False, 2 - 2 * side, 1 - side),
            )
            for b in (-1, 0, 1)
        ]

    def force_measure(n, m):
        cell, near = force_blocks(n)
        ghost, index, row, column = near[m]
        columns = (ghost_jcols if ghost else jcols)[row * COLS + column + 2]
        put_distances(dist, m, rows_of(irows, cell), scales[0, index], columns)

    def gather_sums(n, slopes):
        _, near = force_blocks(n)
        total = jnp.zeros((DEPTH, 256), F32)
        for m in range(9):
            ghost, index, row, column = near[m]
            at = row * PLACES + place_of(column)
            table = ghost_crows if ghost else crows
            table = table[pl.ds(pl.multiple_of(at * TERMS, TERMS), TERMS), :]
            left_side = jnp.concatenate(parts_of(table * scales[1, index, 0:TERMS, :], 2), axis=0)
            left_side = left_side.astype(BF16)
            total = total + jnp.dot(
                jnp.concatenate([left_side, left_side], axis=1),
                slopes[256 * m : 256 * (m + 1), :],
                preferred_element_type=F32,
            )
        total = total[0:16] + total[16:32]
        for half in range(2):
            at = pl.ds(pl.multiple_of(n * 16, 16), 16)
            sums[half, at, :] = total[:, 128 * half : 128 * (half + 1)]

    def put_slopes(n, slopes):
        following = jnp.minimum(n + 1, 15)
        for m in range(9):
            for at in range(0, 128, 32):
                y = jnp.maximum(dist[m, at : at + 32, :], 1e-12)
                inverse = lax.rsqrt(y)
                q = y * inverse
                reach = jnp.maximum(2.0 - q, 0.0)
                slope = jnp.where(y < 1.0, 4.0 - 3.0 * q, reach * reach * inverse)
                soft = lax.rsqrt(y + 4.0 * SOFTENING)
                damped = slope * (y * (soft * soft))
                both = jnp.concatenate([slope, damped], axis=1)
                high = both.astype(BF16)
                base = 256 * m + at
                slopes[base : base + 32, :] = high
                slopes[base + 128 : base + 160, :] = (both - high.astype(F32)).astype(BF16)
            force_measure(following, m)

    def force_step(n, carry):
        gather_sums(jnp.maximum(2 * n - 1, 0), odd_slopes)
        put_slopes(2 * n, even_slopes)
        gather_sums(2 * n, even_slopes)
        put_slopes(2 * n + 1, odd_slopes)
        return carry

    for m in range(9):
        force_measure(0, m)
    lax.fori_loop(0, 8, force_step, 0)
    gather_sums(15, odd_slopes)

    for row in range(2):
        mass = fields[row, 6, 0:8, :]
        valid = mass > 0.0
        rho = rhos[row * PLACES : row * PLACES + 8, :]
        density[row] = jnp.where(valid, rho, 0.0)
        inverse_rho = 1.0 / jnp.where(valid, rho, 1.0)

        def term(k, half):
            return sums[half, pl.ds(row * 128 + k, 8, stride=16), :]

        mass_sum, share_sum, drag_sum = term(0, 0), term(6, 0), term(6, 1)
        pressure_scale = -3.0 * KERNEL_NORM * -SOUND_SQ * 0.5
        viscous_scale = -3.0 * KERNEL_NORM * 2.0 * VISCOSITY
        for f in range(3):
            high, low = parts_of(2.0 * fields[row, f, 0:8, :] - 1.0, 2)
            x = high + low
            first = x * mass_sum - term(1 + f, 0)
            second = x * share_sum - term(7 + f, 0)
            if f < 2:
                first = first - 2.0 * term(4 + f, 0)
                second = second - 2.0 * term(10 + f, 0)
            viscous = fields[row, 3 + f, 0:8, :] * drag_sum - term(12 + f, 1)
            value = pressure_scale * (first * inverse_rho + second)
            value = value + viscous_scale * viscous * inverse_rho
            accel[row, f] = jnp.where(valid, value, 0.0)


def scratch_of(tables, rows):
    return [
        pltpu.VMEM((t.shape[0] // 2 * rows, *t.shape[1:]), t.dtype) for t in tables
    ]


def params(mib):
    return pltpu.CompilerParams(vmem_limit_bytes=mib * 2**20)


def local(rows_axis, columns_axis, position, velocity, particle_mass, cell_counts, shear_shift):
    slabs, blocks = lax.axis_size(rows_axis), lax.axis_size(columns_axis)
    axes = (rows_axis, columns_axis)
    half = blocks // 2
    slab = lax.axis_index(rows_axis)
    past = shear_shift[0] - half * particle_mass.shape[1]

    ring = [(i, (i + 1) % blocks) for i in range(blocks)]
    fields = jnp.concatenate(
        [
            jnp.transpose(position, (0, 3, 1, 2)),
            jnp.transpose(velocity, (0, 3, 1, 2)),
            particle_mass[:, None],
        ],
        axis=1,
    )
    field = lax.broadcasted_iota(jnp.int32, fields.shape, 1)
    slot = lax.broadcasted_iota(jnp.int32, fields.shape, 3)
    fields = jnp.where((field < 6) | (slot < cell_counts[:, None, :, None]), fields, 0.0)
    shapes = (*TABLES, jax.ShapeDtypeStruct((2 * PLACES, 128), F32))

    def tables_call(kernel, run, inputs, tables, blocks):
        count = len(inputs) + 1
        return pl.pallas_call(
            kernel,
            out_shape=shapes,
            in_specs=[SMEM] + [VMEM] * (len(inputs) + len(tables)),
            out_specs=[VMEM] * 5,
            scratch_shapes=[
                pltpu.VMEM((2 * PLACES * DEPTH, 128), F32),
                pltpu.VMEM((1, 9, DEPTH, 128), F32),
                pltpu.VMEM((blocks, 128, 128), F32),
            ],
            input_output_aliases={count + n: n for n in range(len(tables))},
            compiler_params=params(8),
            cost_estimate=pl.CostEstimate(
                flops=100_000_000, bytes_accessed=4_000_000, transcendentals=1_000_000
            ),
        )(run.astype(jnp.int32)[None], *inputs, *tables)

    block = lax.axis_index(columns_axis)
    edge = (slab == 0) | (slab == slabs - 1)
    corner = (block == 0) & (slab == 0)
    ahead, late = (block == 0) & ~corner, edge & (block >= half)
    own_now = [ahead, ~(ahead | late | corner), late, corner]
    beside_now = [~corner, corner]

    def own_work(which, tables):
        return tables_call(own_kernel, own_now[which], (fields,), tables, 6)

    def beside_work(which, tables):
        return tables_call(beside_kernel, beside_now[which], (left, right), tables, 8)

    left = lax.ppermute(fields, columns_axis, ring)
    tables = own_work(0, ())
    right = lax.ppermute(fields, columns_axis, [(j, i) for i, j in ring])
    tables = own_work(1, tables)

    odd = lax.rem(slab, 2)
    start = 6 + jnp.where(slab == slabs - 1, past, jnp.where(slab == 0, -past, 0))
    info = jnp.stack([odd, start]).astype(jnp.int32)
    sent = jax.ShapeDtypeStruct((SENT, 128), F32)
    far, same = pl.pallas_call(
        window_kernel,
        out_shape=(sent, sent),
        in_specs=[SMEM, VMEM, VMEM, VMEM],
        out_specs=(VMEM, VMEM),
        compiler_params=params(4),
        name="window",
    )(info, left, fields, right)

    same_pairs, far_pairs = [], []
    for s in range(slabs):
        for b in range(blocks):
            me = s * blocks + b
            same_pairs.append((me, (s + 1 if s % 2 == 0 else s - 1) * blocks + b))
            other, to = (s - 1, b) if s % 2 == 0 else (s + 1, b)
            if other < 0 or other >= slabs:
                other, to = other % slabs, (b + half) % blocks
            far_pairs.append((me, other * blocks + to))
    far = lax.ppermute(far, axes, far_pairs)
    tables = own_work(2, tables)
    tables = beside_work(0, tables)
    same = lax.ppermute(same, axes, same_pairs)
    tables = own_work(3, tables)
    tables = beside_work(1, tables)

    jump = jnp.where(slab == slabs - 1, SHEAR_JUMP, jnp.where(slab == 0, -SHEAR_JUMP, 0.0))
    density, accel = pl.pallas_call(
        late_kernel,
        out_shape=(
            jax.ShapeDtypeStruct((2, 8, 128), F32),
            jax.ShapeDtypeStruct((2, 3, 8, 128), F32),
        ),
        in_specs=[SMEM, SMEM] + [VMEM] * 7,
        out_specs=(VMEM, VMEM),
        scratch_shapes=[
            *scratch_of(TABLES[:1], 4),
            *scratch_of(TABLES[1:2], 2),
            *scratch_of(TABLES[2:], 4),
            pltpu.VMEM((4 * PLACES * DEPTH, 128), F32),
            pltpu.VMEM((2, 9, DEPTH, 128), F32),
            pltpu.VMEM((2 * PLACES, 128), F32),
            pltpu.VMEM((2 * PLACES, 128), F32),
            pltpu.VMEM((2 * PLACES * TERMS, 128), F32),
            pltpu.VMEM((2 * PLACES * TERMS, 128), F32),
            pltpu.VMEM((12, 128, 128), F32),
            pltpu.VMEM((2, 16 * 16, 128), F32),
            pltpu.VMEM((9 * 256, 256), BF16),
            pltpu.VMEM((9 * 256, 256), BF16),
        ],
        compiler_params=params(24),
        name="late",
    )(info, jump.astype(F32)[None], far, same, *tables)
    return (density, jnp.transpose(accel, (0, 2, 3, 1)))


def solution(mesh):
    placed = (
        P("gy", "gx", None, None),
        P("gy", "gx", None, None),
        P("gy", "gx", None),
        P("gy", "gx"),
        P(),
    )

    def step(*args):
        return local("gy", "gx", *args)

    return jax.shard_map(
        step,
        mesh=mesh,
        in_specs=placed,
        out_specs=(P("gy", "gx", None), P("gy", "gx", None, None)),
        check_vma=False,
    )
```
